8 devices in a mesh: dp: 1 (over z), tp: 2 (over y), cp: 4 (over x, core).
Axes of the slice: x: 2, y: 2, z: 1, core: 2. Of those that a mesh axis runs over, the one named last changes fastest.
Arguments:
- hidden: bfloat16 [32, 32, 2048], P('dp')
- prefix_len: int32 [32], P('dp')
- k_cache: bfloat16 [32, 8192, 8, 128], P('dp', 'cp', 'tp')
- v_cache: bfloat16 [32, 8192, 8, 128], P('dp', 'cp', 'tp')
- attn_norm: bfloat16 [2048], replicated
- w_q: bfloat16 [2048, 2048], P(None, 'tp')
- w_k: bfloat16 [2048, 1024], P(None, 'tp')
- w_v: bfloat16 [2048, 1024], P(None, 'tp')
- w_o: bfloat16 [2048, 2048], P('tp')
- q_norm: bfloat16 [128], replicated
- k_norm: bfloat16 [128], replicated
Outputs:
- output 1: bfloat16 [32, 32, 2048], P('dp')
- output 2: bfloat16 [32, 32, 8, 128], P('dp', None, 'tp')
- output 3: bfloat16 [32, 32, 8, 128], P('dp', None, 'tp')
All inputs are finite; a program needn't handle non-finite values.
Results may differ from the reference program's by a relative error of at most 0.00372417.
Values sent between devices are 32-bit elements.
A program may use at most 1 GiB of HBM per device.

```python
import jax
import jax.numpy as jnp
from jax import lax

NUM_SEQ = 32
NEW_TOKENS = 32
CACHE_LEN = 8192
D_MODEL = 2048
N_HEADS = 16
KV_HEADS = 8
HEAD_DIM = 128


def rms_scale(tensor, norm_gain):
    mean_sq = jnp.mean(jnp.square(tensor), axis=-1, keepdims=True)
    return tensor * lax.rsqrt(mean_sq + 1e-6) * norm_gain


def rope_apply(tensor, positions):
    half_dim = HEAD_DIM // 2
    inv_freq = 1.0 / (1000000.0 ** (jnp.arange(half_dim, dtype=jnp.float32) * 2.0 / HEAD_DIM))
    angles = positions.astype(jnp.float32)[..., None] * inv_freq
    cos_t = jnp.cos(angles)[..., None, :]
    sin_t = jnp.sin(angles)[..., None, :]
    lead_half = tensor[..., :half_dim]
    tail_half = tensor[..., half_dim:]
    return jnp.concatenate([lead_half * cos_t - tail_half * sin_t, tail_half * cos_t + lead_half * sin_t], axis=-1)


def smooth_field(key, amplitude):
    n_freq = 4
    coords = (jnp.arange(CACHE_LEN, dtype=jnp.float32) + 0.5) / CACHE_LEN
    angles = jnp.pi * coords[:, None] * jnp.arange(1, n_freq + 1, dtype=jnp.float32)[None, :]
    cos_basis = jnp.concatenate([jnp.cos(angles), jnp.sin(angles)], axis=1)
    coeffs = jax.random.normal(key, (NUM_SEQ, 2 * n_freq, KV_HEADS, HEAD_DIM), jnp.float32) * (amplitude / n_freq ** 0.5)
    return jnp.einsum('pf,bfke->bpke', cos_basis, coeffs)


def setup_inputs(seed: int = 0, part: int = 0) -> dict:
    shared = jax.random.split(jax.random.key(seed), 8)
    part_keys = jax.random.split(jax.random.fold_in(jax.random.key(seed + 1), part), 8)
    cache_shape = (NUM_SEQ, CACHE_LEN, KV_HEADS, HEAD_DIM)
    len_draw = jax.random.randint(part_keys[1], (NUM_SEQ,), 0, CACHE_LEN + 1)
    full_at = jax.random.randint(part_keys[2], (), 0, NUM_SEQ)
    prefix_len = jnp.where(jnp.arange(NUM_SEQ) == full_at, CACHE_LEN, len_draw).astype(jnp.int32)
    k_cache = smooth_field(part_keys[3], 2.0) + 0.5 * jax.random.normal(part_keys[4], cache_shape, jnp.float32)
    v_cache = smooth_field(part_keys[5], 1.0) + 0.5 * jax.random.normal(part_keys[6], cache_shape, jnp.float32)
    q_width = N_HEADS * HEAD_DIM
    kv_width = KV_HEADS * HEAD_DIM
    return {
        'hidden': jax.random.normal(part_keys[0], (NUM_SEQ, NEW_TOKENS, D_MODEL), jnp.float32).astype(jnp.bfloat16),
        'prefix_len': prefix_len,
        'k_cache': k_cache.astype(jnp.bfloat16),
        'v_cache': v_cache.astype(jnp.bfloat16),
        'attn_norm': (1.0 + 0.4 * jax.random.normal(shared[0], (D_MODEL,), jnp.float32)).astype(jnp.bfloat16),
        'w_q': (jax.random.normal(shared[1], (D_MODEL, q_width), jnp.float32) * D_MODEL ** -0.5).astype(jnp.bfloat16),
        'w_k': (jax.random.normal(shared[2], (D_MODEL, kv_width), jnp.float32) * D_MODEL ** -0.5).astype(jnp.bfloat16),
        'w_v': (jax.random.normal(shared[3], (D_MODEL, kv_width), jnp.float32) * D_MODEL ** -0.5).astype(jnp.bfloat16),
        'w_o': (jax.random.normal(shared[4], (q_width, D_MODEL), jnp.float32) * q_width ** -0.5).astype(jnp.bfloat16),
        'q_norm': (1.0 + 0.4 * jax.random.normal(shared[5], (HEAD_DIM,), jnp.float32)).astype(jnp.bfloat16),
        'k_norm': (1.0 + 0.4 * jax.random.normal(shared[6], (HEAD_DIM,), jnp.float32)).astype(jnp.bfloat16),
    }


def reference(hidden, prefix_len, k_cache, v_cache, attn_norm, w_q, w_k, w_v, w_o, q_norm, k_norm):
    group_size = N_HEADS // KV_HEADS
    flat_rows = hidden.reshape(NUM_SEQ * NEW_TOKENS, D_MODEL)
    normed = rms_scale(flat_rows.astype(jnp.float32), attn_norm.astype(jnp.float32)).astype(jnp.bfloat16)
    q_lin = jnp.dot(normed, w_q, preferred_element_type=jnp.float32).astype(jnp.bfloat16)
    k_lin = jnp.dot(normed, w_k, preferred_element_type=jnp.float32).astype(jnp.bfloat16)
    v_lin = jnp.dot(normed, w_v, preferred_element_type=jnp.float32).astype(jnp.bfloat16)
    positions = prefix_len[:, None] + jnp.arange(NEW_TOKENS, dtype=jnp.int32)[None, :]
    q_heads = q_lin.reshape(NUM_SEQ, NEW_TOKENS, N_HEADS, HEAD_DIM).astype(jnp.float32)
    k_heads = k_lin.reshape(NUM_SEQ, NEW_TOKENS, KV_HEADS, HEAD_DIM).astype(jnp.float32)
    q_rot = rope_apply(rms_scale(q_heads, q_norm.astype(jnp.float32)), positions).astype(jnp.bfloat16)
    k_new = rope_apply(rms_scale(k_heads, k_norm.astype(jnp.float32)), positions).astype(jnp.bfloat16)
    v_new = v_lin.reshape(NUM_SEQ, NEW_TOKENS, KV_HEADS, HEAD_DIM)
    causal = jnp.arange(NEW_TOKENS)[:, None] >= jnp.arange(NEW_TOKENS)[None, :]
    score_scale = HEAD_DIM ** -0.5

    def one_sequence(operands):
        q_seq, k_seq, v_seq, kc_seq, vc_seq, seq_len = operands
        cache_ok = jnp.arange(CACHE_LEN) < seq_len
        key_mask = jnp.concatenate([jnp.broadcast_to(cache_ok[None, :], (NEW_TOKENS, CACHE_LEN)), causal], axis=1)

        def one_head_group(group_ops):
            q_grp, key_all, val_all = group_ops
            scores = jnp.einsum('cgd,kd->gck', q_grp.astype(jnp.float32), key_all.astype(jnp.float32)) * score_scale
            scores = jnp.where(key_mask[None], scores, -jnp.inf)
            prob_mat = jax.nn.softmax(scores, axis=-1)
            return jnp.einsum('gck,kd->cgd', prob_mat, val_all.astype(jnp.float32))

        key_all = jnp.concatenate([kc_seq, k_seq], axis=0).transpose(1, 0, 2)
        val_all = jnp.concatenate([vc_seq, v_seq], axis=0).transpose(1, 0, 2)
        q_grp = q_seq.reshape(NEW_TOKENS, KV_HEADS, group_size, HEAD_DIM).transpose(1, 0, 2, 3)
        out_grp = lax.map(one_head_group, (q_grp, key_all, val_all))
        return out_grp.transpose(1, 0, 2, 3).reshape(NEW_TOKENS, N_HEADS * HEAD_DIM)

    attn_seq = lax.map(one_sequence, (q_rot, k_new, v_new, k_cache, v_cache, prefix_len))
    attn_rows = attn_seq.reshape(NUM_SEQ * NEW_TOKENS, N_HEADS * HEAD_DIM).astype(jnp.bfloat16)
    block_out = flat_rows.astype(jnp.float32) + jnp.dot(attn_rows, w_o, preferred_element_type=jnp.float32)
    return block_out.astype(jnp.bfloat16).reshape(NUM_SEQ, NEW_TOKENS, D_MODEL), k_new, v_new
```

```python
import functools

import jax
import jax.numpy as jnp
from jax import lax
from jax.experimental import pallas as pl
from jax.experimental.pallas import tpu as pltpu
from jax.sharding import PartitionSpec as P

HEAD_DIM = 128
NEG = -3e38
FLOOR = -1e38
LOG2E = 1.4426950408889634
NBUF = 3
CHUNK = 512


def rms_scale(tensor, norm_gain):
    mean_sq = jnp.mean(jnp.square(tensor), axis=-1, keepdims=True)
    return tensor * lax.rsqrt(mean_sq + 1e-6) * norm_gain


def rope_apply(tensor, positions):
    half_dim = HEAD_DIM // 2
    inv_freq = 1.0 / (1000000.0 ** (jnp.arange(half_dim, dtype=jnp.float32) * 2.0 / HEAD_DIM))
    angles = positions.astype(jnp.float32)[..., None] * inv_freq
    cos_t = jnp.cos(angles)[..., None, :]
    sin_t = jnp.sin(angles)[..., None, :]
    lead_half = tensor[..., :half_dim]
    tail_half = tensor[..., half_dim:]
    return jnp.concatenate([lead_half * cos_t - tail_half * sin_t, tail_half * cos_t + lead_half * sin_t], axis=-1)


def project_new(hidden, attn_norm, w_q, w_k, w_v, q_norm, k_norm, prefix_len):
    n_seq, n_new, d_model = hidden.shape
    kv_count = w_k.shape[1] // HEAD_DIM
    head_count = w_q.shape[1] // HEAD_DIM
    normed = rms_scale(hidden.astype(jnp.float32), attn_norm.astype(jnp.float32)).astype(jnp.bfloat16)
    q_lin = jnp.einsum('bce,ef->bcf', normed, w_q, preferred_element_type=jnp.float32).astype(jnp.bfloat16)
    k_lin = jnp.einsum('bce,ef->bcf', normed, w_k, preferred_element_type=jnp.float32).astype(jnp.bfloat16)
    v_lin = jnp.einsum('bce,ef->bcf', normed, w_v, preferred_element_type=jnp.float32).astype(jnp.bfloat16)
    positions = prefix_len[:, None] + jnp.arange(n_new, dtype=jnp.int32)[None, :]
    q_heads = q_lin.reshape(n_seq, n_new, head_count, HEAD_DIM).astype(jnp.float32)
    k_heads = k_lin.reshape(n_seq, n_new, kv_count, HEAD_DIM).astype(jnp.float32)
    q_rot = rope_apply(rms_scale(q_heads, q_norm.astype(jnp.float32)), positions).astype(jnp.bfloat16)
    k_new = rope_apply(rms_scale(k_heads, k_norm.astype(jnp.float32)), positions).astype(jnp.bfloat16)
    v_new = v_lin.reshape(n_seq, n_new, kv_count, HEAD_DIM)
    return q_rot, k_new, v_new


def head_rows(ref, start, count, head):
    return ref[pl.ds(start * 4 + head, count, stride=4), :]


def pair_rows(ref, start, count, pair):
    return jnp.concatenate([head_rows(ref, start, count, 2 * pair), head_rows(ref, start, count, 2 * pair + 1)], axis=1)


def query_weights(q_ref, b, pair):
    def head(h):
        return jnp.concatenate([q_ref[b, :, (2 * h + g) * 128:(2 * h + g + 1) * 128] for g in range(2)], axis=0)
    zero = jnp.zeros((64, 128), jnp.bfloat16)
    top = jnp.concatenate([head(2 * pair), zero], axis=1)
    low = jnp.concatenate([zero, head(2 * pair + 1)], axis=1)
    return jnp.concatenate([top, low], axis=0).T


def score_pass(q_ref, kn_ref, kbuf, scores, own_scores, b, limit, own):
    tops = []
    row = lax.broadcasted_iota(jnp.int32, (CHUNK, 128), 0)
    own_row = lax.broadcasted_iota(jnp.int32, (32, 128), 0)
    token = lax.broadcasted_iota(jnp.int32, (32, 128), 1) % 32
    for pair in range(2):
        wq = query_weights(q_ref, b, pair)
        top = jnp.full((8, 128), FLOOR, jnp.float32)
        for c in range(2048 // CHUNK):
            s = jnp.dot(pair_rows(kbuf, c * CHUNK, CHUNK, pair), wq, preferred_element_type=jnp.float32)
            s = jnp.where(row < limit - c * CHUNK, s, NEG)
            scores[pair, pl.ds(c * CHUNK, CHUNK), :] = s
            top = jnp.maximum(top, jnp.max(s.reshape(CHUNK // 8, 8, 128), axis=0))
        s = jnp.dot(pair_rows(kn_ref.at[b], 0, 32, pair), wq, preferred_element_type=jnp.float32)
        s = jnp.where(own_row <= token - own, s, NEG)
        own_scores[pair] = s
        top = jnp.maximum(top, jnp.max(s.reshape(4, 8, 128), axis=0))
        tops.append(jnp.max(top, axis=0, keepdims=True))
    return tops


def value_pass(vn_ref, vbuf, scores, own_scores, tops, b):
    scale = HEAD_DIM ** -0.5 * LOG2E
    outs = []
    for pair in range(2):
        top = tops[pair]
        total = jnp.zeros((8, 128), jnp.float32)
        out = jnp.zeros((128, 256), jnp.float32)
        for c in range(2048 // CHUNK):
            p = jnp.exp2((scores[pair, pl.ds(c * CHUNK, CHUNK), :] - top) * scale)
            total = total + jnp.sum(p.reshape(CHUNK // 8, 8, 128), axis=0)
            out = out + jnp.dot(p.astype(jnp.bfloat16).T, pair_rows(vbuf, c * CHUNK, CHUNK, pair), preferred_element_type=jnp.float32)
        p = jnp.exp2((own_scores[pair] - top) * scale)
        total = total + jnp.sum(p.reshape(4, 8, 128), axis=0)
        out = out + jnp.dot(p.astype(jnp.bfloat16).T, pair_rows(vn_ref.at[b], 0, 32, pair), preferred_element_type=jnp.float32)
        outs.append((out, jnp.sum(total, axis=0, keepdims=True)))
    return outs


def stat_tile(rows, lane0):
    lane = lax.broadcasted_iota(jnp.int32, (32, 128), 1)
    tile = jnp.zeros((32, 128), jnp.float32)
    for pair in range(2):
        col = jnp.broadcast_to(rows[pair], (128, 128)).T
        for i in range(4):
            tile = jnp.where(lane == lane0 + 4 * pair + i, col[i * 32:(i + 1) * 32], tile)
    return tile


def attend_kernel(limit_ref, q_ref, kn_ref, vn_ref, k_hbm, v_hbm, w_ref, kbuf, vbuf, scores, own_scores, ksem, vsem):
    n_seq = q_ref.shape[0]

    def copies(b):
        slot = lax.rem(b, NBUF)
        return (pltpu.make_async_copy(k_hbm.at[b], kbuf.at[slot], ksem.at[slot]),
                pltpu.make_async_copy(v_hbm.at[b], vbuf.at[slot], vsem.at[slot]))

    for b in range(NBUF - 1):
        for copy in copies(b):
            copy.start()
    own = limit_ref[n_seq]
    copies(0)[0].wait()
    tops = score_pass(q_ref, kn_ref, kbuf.at[0], scores.at[0], own_scores.at[0], 0, limit_ref[0], own)

    def step(b, tops, last):
        slot = lax.rem(b, NBUF)
        par = lax.rem(b, 2)
        copies(b)[1].wait()
        if not last:
            nxt = lax.rem(b + 1, NBUF)
            copies(b + 1)[0].wait()

            @pl.when(b + NBUF - 1 < n_seq)
            def _():
                for copy in copies(b + NBUF - 1):
                    copy.start()
            new_tops = score_pass(q_ref, kn_ref, kbuf.at[nxt], scores.at[1 - par], own_scores.at[1 - par], b + 1, limit_ref[b + 1], own)
        outs = value_pass(vn_ref, vbuf.at[slot], scores.at[par], own_scores.at[par], tops, b)
        for pair in range(2):
            out = outs[pair][0]
            for i in range(4):
                head = 4 * pair + i
                w_ref[b, :, head * 128:(head + 1) * 128] = out[i * 32:(i + 1) * 32, (i // 2) * 128:(i // 2 + 1) * 128]
        w_ref[b, :, 1024:1152] = stat_tile(tops, 0) + stat_tile([o[1] for o in outs], 8)
        return None if last else tuple(new_tops)

    tops = lax.fori_loop(0, n_seq - 1, lambda b, t: step(b, t, False), tuple(tops))
    step(n_seq - 1, tops, True)


def attend(q, k_new, v_new, k_cache, v_cache, limits):
    n_seq = q.shape[0]
    rows = k_cache.shape[1] * 4
    vmem = pl.BlockSpec(memory_space=pltpu.VMEM)
    return pl.pallas_call(
        attend_kernel,
        out_shape=jax.ShapeDtypeStruct((n_seq, 32, 1152), jnp.float32),
        in_specs=[pl.BlockSpec(memory_space=pltpu.SMEM), vmem, vmem, vmem, pl.BlockSpec(memory_space=pl.ANY), pl.BlockSpec(memory_space=pl.ANY)],
        out_specs=vmem,
        scratch_shapes=[
            pltpu.VMEM((NBUF, rows, 128), jnp.bfloat16),
            pltpu.VMEM((NBUF, rows, 128), jnp.bfloat16),
            pltpu.VMEM((2, 2, 2048, 128), jnp.float32),
            pltpu.VMEM((2, 2, 32, 128), jnp.float32),
            pltpu.SemaphoreType.DMA((NBUF,)),
            pltpu.SemaphoreType.DMA((NBUF,)),
        ],
        compiler_params=pltpu.CompilerParams(vmem_limit_bytes=48 * 1024 * 1024),
        cost_estimate=pl.CostEstimate(flops=17_000_000_000, bytes_accessed=140_000_000, transcendentals=17_000_000),
    )(limits, q, k_new.reshape(n_seq, 128, 128), v_new.reshape(n_seq, 128, 128), k_cache.reshape(n_seq, rows, 128), v_cache.reshape(n_seq, rows, 128))


def solution(mesh):
    def per_device(hidden, prefix_len, k_cache, v_cache, attn_norm, w_q, w_k, w_v, w_o, q_norm, k_norm):
        n_seq, n_new, d_model = hidden.shape
        cp = lax.axis_index('cp')
        tp = lax.axis_index('tp')
        q_rot, k_new, v_new = project_new(hidden, attn_norm, w_q, w_k, w_v, q_norm, k_norm, prefix_len)
        limits = jnp.concatenate([prefix_len - cp * 2048, jnp.where(cp == 3, 0, 64)[None]]).astype(jnp.int32)
        w = attend(q_rot.reshape(n_seq, n_new, 1024), k_new, v_new, k_cache, v_cache, limits)

        def swap(array, axis, bit):
            count = mesh.shape[axis]
            return lax.ppermute(array, axis, [(i, i ^ bit) for i in range(count)])

        def keep_send(array, which):
            half = array.shape[1] // 2
            first, second = array[:, :half], array[:, half:]
            return jnp.where(which == 0, first, second), jnp.where(which == 0, second, first)

        def merge(a, b):
            ma, mb = a[..., 1024:1032], b[..., 1024:1032]
            m = jnp.maximum(ma, mb)
            scale = HEAD_DIM ** -0.5 * LOG2E
            fa, fb = jnp.exp2((ma - m) * scale), jnp.exp2((mb - m) * scale)
            shape = a.shape[:2] + (8, 128)
            w = a[..., :1024].reshape(shape) * fa[..., None] + b[..., :1024].reshape(shape) * fb[..., None]
            l = a[..., 1032:1040] * fa + b[..., 1032:1040] * fb
            return w, m, l

        def pack(w, m, l):
            rest = jnp.zeros(m.shape[:2] + (112,), jnp.float32)
            return jnp.concatenate([w.reshape(w.shape[:2] + (1024,)), m, l, rest], axis=-1)

        keep, send = keep_send(w, cp % 2)
        half = pack(*merge(keep, swap(send, 'cp', 1)))
        keep, send = keep_send(half, cp // 2)
        w4, _, l4 = merge(keep, swap(send, 'cp', 2))
        o = (w4 / l4[..., None]).astype(jnp.bfloat16).reshape(n_seq * 8, 1024)
        part = jnp.dot(o, w_o, preferred_element_type=jnp.float32)
        first, second = part[:, :1024], part[:, 1024:]
        mine = jnp.where(tp == 0, first, second) + swap(jnp.where(tp == 0, second, first), 'tp', 1)
        ay = swap(mine, 'tp', 1)
        ax = swap(mine, 'cp', 2)
        dh = mine.shape[0] // 2
        d0 = swap(ay[:dh], 'cp', 2)
        d1 = swap(ax[dh:], 'tp', 1)
        diag = jnp.concatenate([d0, d1], axis=0)
        x_mine = jnp.concatenate([jnp.where(tp == 0, mine, ay), jnp.where(tp == 0, ay, mine)], axis=1)
        x_other = jnp.concatenate([jnp.where(tp == 0, ax, diag), jnp.where(tp == 0, diag, ax)], axis=1)
        x_mine = x_mine.reshape(n_seq, 8, d_model)
        x_other = x_other.reshape(n_seq, 8, d_model)
        x = cp // 2
        core = jnp.concatenate([jnp.where(x == 0, x_mine, x_other), jnp.where(x == 0, x_other, x_mine)], axis=1)
        peer = swap(core, 'cp', 1)
        k = cp % 2
        total = jnp.concatenate([jnp.where(k == 0, core, peer), jnp.where(k == 0, peer, core)], axis=1)
        block_out = (hidden.astype(jnp.float32) + total).astype(jnp.bfloat16)
        return block_out, k_new, v_new

    cache_spec = P('dp', 'cp', 'tp', None)
    arg_specs = (P('dp', None, None), P('dp'), cache_spec, cache_spec, P(None), P(None, 'tp'), P(None, 'tp'), P(None, 'tp'), P('tp', None), P(None), P(None))
    out_specs = (P('dp', None, None), P('dp', None, 'tp', None), P('dp', None, 'tp', None))
    return jax.shard_map(per_device, mesh=mesh, in_specs=arg_specs, out_specs=out_specs, check_vma=False)
```

```python
import functools

import jax
import jax.numpy as jnp
from jax import lax
from jax.experimental import pallas as pl
from jax.experimental.pallas import tpu as pltpu
from jax.sharding import PartitionSpec as P

HEAD_DIM = 128
NEG = -3e38
FLOOR = -1e38
LOG2E = 1.4426950408889634
NBUF = 3
CHUNK = 512


def rms_scale(tensor, norm_gain):
    mean_sq = jnp.mean(jnp.square(tensor), axis=-1, keepdims=True)
    return tensor * lax.rsqrt(mean_sq + 1e-6) * norm_gain


def rope_apply(tensor, positions):
    half_dim = HEAD_DIM // 2
    inv_freq = 1.0 / (1000000.0 ** (jnp.arange(half_dim, dtype=jnp.float32) * 2.0 / HEAD_DIM))
    angles = positions.astype(jnp.float32)[..., None] * inv_freq
    cos_t = jnp.cos(angles)[..., None, :]
    sin_t = jnp.sin(angles)[..., None, :]
    lead_half = tensor[..., :half_dim]
    tail_half = tensor[..., half_dim:]
    return jnp.concatenate([lead_half * cos_t - tail_half * sin_t, tail_half * cos_t + lead_half * sin_t], axis=-1)


def project_new(hidden, attn_norm, w_q, w_k, w_v, q_norm, k_norm, prefix_len):
    n_seq, n_new, d_model = hidden.shape
    kv_count = w_k.shape[1] // HEAD_DIM
    head_count = w_q.shape[1] // HEAD_DIM
    normed = rms_scale(hidden.astype(jnp.float32), attn_norm.astype(jnp.float32)).astype(jnp.bfloat16)
    q_lin = jnp.einsum('bce,ef->bcf', normed, w_q, preferred_element_type=jnp.float32).astype(jnp.bfloat16)
    k_lin = jnp.einsum('bce,ef->bcf', normed, w_k, preferred_element_type=jnp.float32).astype(jnp.bfloat16)
    v_lin = jnp.einsum('bce,ef->bcf', normed, w_v, preferred_element_type=jnp.float32).astype(jnp.bfloat16)
    positions = prefix_len[:, None] + jnp.arange(n_new, dtype=jnp.int32)[None, :]
    q_heads = q_lin.reshape(n_seq, n_new, head_count, HEAD_DIM).astype(jnp.float32)
    k_heads = k_lin.reshape(n_seq, n_new, kv_count, HEAD_DIM).astype(jnp.float32)
    q_rot = rope_apply(rms_scale(q_heads, q_norm.astype(jnp.float32)), positions).astype(jnp.bfloat16)
    k_new = rope_apply(rms_scale(k_heads, k_norm.astype(jnp.float32)), positions).astype(jnp.bfloat16)
    v_new = v_lin.reshape(n_seq, n_new, kv_count, HEAD_DIM)
    return q_rot, k_new, v_new


def head_rows(ref, start, count, head):
    return ref[pl.ds(start * 4 + head, count, stride=4), :]


def pair_rows(ref, start, count, pair):
    return jnp.concatenate([head_rows(ref, start, count, 2 * pair), head_rows(ref, start, count, 2 * pair + 1)], axis=1)


def query_weights(q_ref, b, pair):
    def head(h):
        return jnp.concatenate([q_ref[b, :, (2 * h + g) * 128:(2 * h + g + 1) * 128] for g in range(2)], axis=0)
    zero = jnp.zeros((64, 128), jnp.bfloat16)
    top = jnp.concatenate([head(2 * pair), zero], axis=1)
    low = jnp.concatenate([zero, head(2 * pair + 1)], axis=1)
    return jnp.concatenate([top, low], axis=0).T


def score_pass(q_ref, kn_ref, kbuf, scores, own_scores, b, limit, own):
    tops = []
    row = lax.broadcasted_iota(jnp.int32, (CHUNK, 128), 0)
    own_row = lax.broadcasted_iota(jnp.int32, (32, 128), 0)
    token = lax.broadcasted_iota(jnp.int32, (32, 128), 1) % 32
    for pair in range(2):
        wq = query_weights(q_ref, b, pair)
        top = jnp.full((8, 128), FLOOR, jnp.float32)
        for c in range(2048 // CHUNK):
            s = jnp.dot(pair_rows(kbuf, c * CHUNK, CHUNK, pair), wq, preferred_element_type=jnp.float32)
            s = jnp.where(row < limit - c * CHUNK, s, NEG)
            scores[pair, pl.ds(c * CHUNK, CHUNK), :] = s
            top = jnp.maximum(top, jnp.max(s.reshape(CHUNK // 8, 8, 128), axis=0))
        s = jnp.dot(pair_rows(kn_ref.at[b], 0, 32, pair), wq, preferred_element_type=jnp.float32)
        s = jnp.where(own_row <= token - own, s, NEG)
        own_scores[pair] = s
        top = jnp.maximum(top, jnp.max(s.reshape(4, 8, 128), axis=0))
        tops.append(jnp.max(top, axis=0, keepdims=True))
    return tops


def value_pass(vn_ref, vbuf, scores, own_scores, tops, b):
    scale = HEAD_DIM ** -0.5 * LOG2E
    outs = []
    for pair in range(2):
        top = tops[pair]
        total = jnp.zeros((8, 128), jnp.float32)
        out = jnp.zeros((128, 256), jnp.float32)
        for c in range(2048 // CHUNK):
            p = jnp.exp2((scores[pair, pl.ds(c * CHUNK, CHUNK), :] - top) * scale)
            total = total + jnp.sum(p.reshape(CHUNK // 8, 8, 128), axis=0)
            out = out + jnp.dot(p.astype(jnp.bfloat16).T, pair_rows(vbuf, c * CHUNK, CHUNK, pair), preferred_element_type=jnp.float32)
        p = jnp.exp2((own_scores[pair] - top) * scale)
        total = total + jnp.sum(p.reshape(4, 8, 128), axis=0)
        out = out + jnp.dot(p.astype(jnp.bfloat16).T, pair_rows(vn_ref.at[b], 0, 32, pair), preferred_element_type=jnp.float32)
        outs.append((out, jnp.sum(total, axis=0, keepdims=True)))
    return outs


def stat_tile(rows, lane0):
    lane = lax.broadcasted_iota(jnp.int32, (32, 128), 1)
    tile = jnp.zeros((32, 128), jnp.float32)
    for pair in range(2):
        col = jnp.broadcast_to(rows[pair], (128, 128)).T
        for i in range(4):
            tile = jnp.where(lane == lane0 + 4 * pair + i, col[i * 32:(i + 1) * 32], tile)
    return tile


N_SEQ = 32
BATCH = 4
N_BATCH = N_SEQ // BATCH
LAG_X, LAG_Y, LAG_G, LAG_D, LAG_F = 6, 9, 13, 16, 18
SCALE = HEAD_DIM ** -0.5 * LOG2E
MESH = pl.DeviceIdType.MESH


def merge_parts(a, r):
    sa, sr = a[:, 1024:], r[:, 1024:]
    lane = lax.broadcasted_iota(jnp.int32, sa.shape, 1)
    top = jnp.maximum(sa, sr)
    fa = jnp.where(lane < 8, jnp.exp2((sa - top) * SCALE), 0.0)
    fr = jnp.where(lane < 8, jnp.exp2((sr - top) * SCALE), 0.0)
    total = sa * pltpu.roll(fa, 8, 1) + sr * pltpu.roll(fr, 8, 1)
    parts = []
    for h in range(8):
        cols = slice(h * 128, (h + 1) * 128)
        parts.append(a[:, cols] * fa[:, h:h + 1] + r[:, cols] * fr[:, h:h + 1])
    return parts, jnp.where(lane < 8, top, total)


def block_kernel(limit_ref, q_ref, kn_ref, vn_ref, x_ref, wo_ref, k_hbm, v_hbm, out_ref,
                 kbuf, vbuf, scores, own_scores, tops_ref, part, part_in, half, half_in, proj, proj_in, gath,
                 ksem, vsem, d_send, d_recv, x_send, x_recv, y_send, y_recv, gx_send, gx_recv, gy_send, gy_recv,
                 dx_send, dx_recv, dy_send, dy_recv, c_send, c_recv):
    dp, tp, cp = lax.axis_index('dp'), lax.axis_index('tp'), lax.axis_index('cp')
    x, k = cp // 2, cp % 2
    core_peer = (dp, tp, cp + 1 - 2 * k)
    x_peer = (dp, tp, cp + 2 - 4 * x)
    y_peer = (dp, 1 - tp, cp)

    barrier = pltpu.get_barrier_semaphore()
    for peer in (core_peer, x_peer, y_peer):
        pl.semaphore_signal(barrier, inc=1, device_id=peer, device_id_type=MESH)

    def copies(b):
        slot = lax.rem(b, NBUF)
        return (pltpu.make_async_copy(k_hbm.at[b], kbuf.at[slot], ksem.at[slot]),
                pltpu.make_async_copy(v_hbm.at[b], vbuf.at[slot], vsem.at[slot]))

    def remote(src, dst, send, recv, peer):
        return pltpu.make_async_remote_copy(src_ref=src, dst_ref=dst, send_sem=send, recv_sem=recv, device_id=peer, device_id_type=MESH)

    def core_copy(b):
        return remote(part.at[b, pl.ds(pl.multiple_of((1 - k) * 16, 16), 16)], part_in.at[b], d_send.at[b], d_recv.at[b], core_peer)

    def x_copy(b):
        return remote(half.at[b, pl.ds(pl.multiple_of((1 - x) * 8, 8), 8)], half_in.at[b], x_send.at[b], x_recv.at[b], x_peer)

    def y_copy(n):
        return remote(proj.at[n, 1 - tp], proj_in.at[n], y_send.at[n], y_recv.at[n], y_peer)

    def slot_of(xx, yy, kk):
        return (xx * 2 + yy) * 2 + kk

    mine = slot_of(x, tp, k)
    from_x = slot_of(1 - x, tp, k)
    from_y = slot_of(x, 1 - tp, k)
    diag = slot_of(1 - x, 1 - tp, k)

    def gx_copy(n):
        return remote(gath.at[mine, n], gath.at[mine, n], gx_send.at[n], gx_recv.at[n], x_peer)

    def gy_copy(n):
        return remote(gath.at[mine, n], gath.at[mine, n], gy_send.at[n], gy_recv.at[n], y_peer)

    def dx_copy(n):
        return remote(gath.at[from_y, n, pl.ds(0, 16)], gath.at[from_y, n, pl.ds(0, 16)], dx_send.at[n], dx_recv.at[n], x_peer)

    def dy_copy(n):
        return remote(gath.at[from_x, n, pl.ds(16, 16)], gath.at[from_x, n, pl.ds(16, 16)], dy_send.at[n], dy_recv.at[n], y_peer)

    def c_copy(n, slot, i):
        return remote(gath.at[slot, n], gath.at[slot, n], c_send.at[i, n], c_recv.at[i, n], core_peer)

    for b in range(NBUF - 1):
        for copy in copies(b):
            copy.start()
    own = limit_ref[N_SEQ]

    def run_scores(b, par):
        tops = score_pass(q_ref, kn_ref, kbuf.at[lax.rem(b, NBUF)], scores.at[par], own_scores.at[par], b, limit_ref[b], own)
        for pair in range(2):
            tops_ref[par, pair] = jnp.broadcast_to(tops[pair], (8, 128))

    copies(0)[0].wait()
    run_scores(0, 0)
    pl.semaphore_wait(barrier, 3)

    def step(it, carry):
        @pl.when(it < N_SEQ)
        def _():
            b, par = it, lax.rem(it, 2)
            copies(b)[1].wait()

            @pl.when(b + 1 < N_SEQ)
            def _():
                copies(b + 1)[0].wait()

            @pl.when(b + NBUF - 1 < N_SEQ)
            def _():
                for copy in copies(b + NBUF - 1):
                    copy.start()

            run_scores(jnp.minimum(b + 1, N_SEQ - 1), 1 - par)
            tops = [tops_ref[par, pair, 0:1, :] for pair in range(2)]
            outs = value_pass(vn_ref, vbuf.at[lax.rem(b, NBUF)], scores.at[par], own_scores.at[par], tops, b)
            for pair in range(2):
                out = outs[pair][0]
                for i in range(4):
                    head = 4 * pair + i
                    part[b, :, head * 128:(head + 1) * 128] = out[i * 32:(i + 1) * 32, (i // 2) * 128:(i // 2 + 1) * 128]
            part[b, :, 1024:1152] = stat_tile(tops, 0) + stat_tile([o[1] for o in outs], 8)
            core_copy(b).start()

        @pl.when((it >= 1) & (it < N_SEQ + 1))
        def _():
            b = it - 1
            core_copy(b).wait_recv()
            parts, stats = merge_parts(part[b, pl.ds(pl.multiple_of(k * 16, 16), 16), :], part_in[b])
            for h in range(8):
                half[b, :, h * 128:(h + 1) * 128] = parts[h]
            half[b, :, 1024:] = stats
            x_copy(b).start()

        def batch_of(lag):
            n = (it - lag) // BATCH
            return n, (it >= lag) & ((it - lag) % BATCH == 0) & (n < N_BATCH)

        n_x, now_x = batch_of(LAG_X)

        @pl.when(now_x)
        def _():
            n = n_x
            for i in range(BATCH):
                x_copy(n * BATCH + i).wait_recv()
            seqs = pl.ds(n * BATCH, BATCH)
            a = half[seqs, pl.ds(pl.multiple_of(x * 8, 8), 8), :].reshape(BATCH * 8, 1152)
            r = half_in[seqs].reshape(BATCH * 8, 1152)
            parts, stats = merge_parts(a, r)
            inv = 1.0 / stats[:, 8:16]
            o = jnp.concatenate([parts[h] * inv[:, h:h + 1] for h in range(8)], axis=1).astype(jnp.bfloat16)
            for y in range(2):
                proj[n, y] = jnp.dot(o, wo_ref[:, y * 1024:(y + 1) * 1024], preferred_element_type=jnp.float32)
            y_copy(n).start()

        n_y, now_y = batch_of(LAG_Y)

        @pl.when(now_y)
        def _():
            n = n_y
            y_copy(n).wait_recv()
            res = x_ref[pl.ds(n * BATCH, BATCH)].reshape(BATCH * 8, 1024).astype(jnp.float32)
            gath[mine, n] = proj[n, tp] + proj_in[n] + res
            gy_copy(n).start()
            gx_copy(n).start()
            c_copy(n, mine, 0).start()

        n_g, now_g = batch_of(LAG_G)

        @pl.when(now_g)
        def _():
            n = n_g
            gy_copy(n).wait_recv()
            dx_copy(n).start()
            c_copy(n, from_y, 1).start()
            gx_copy(n).wait_recv()
            dy_copy(n).start()
            c_copy(n, from_x, 2).start()

        n_d, now_d = batch_of(LAG_D)

        @pl.when(now_d)
        def _():
            n = n_d
            dx_copy(n).wait_recv()
            dy_copy(n).wait_recv()
            c_copy(n, diag, 3).start()

        n_f, now_f = batch_of(LAG_F)

        @pl.when(now_f)
        def _():
            n = n_f
            for i in range(4):
                c_copy(n, mine, i).wait_recv()
            for kk in range(2):
                for y in range(2):
                    lo = gath[slot_of(0, y, kk), n].reshape(BATCH, 8, 1024)
                    hi = gath[slot_of(1, y, kk), n].reshape(BATCH, 8, 1024)
                    out_ref[pl.ds(n * BATCH, BATCH), kk * 16:(kk + 1) * 16, y * 1024:(y + 1) * 1024] = jnp.concatenate([lo, hi], axis=1).astype(jnp.bfloat16)

        return carry

    lax.fori_loop(0, N_SEQ + LAG_F - BATCH + 1, step, 0)

    def drain_seq(b, carry):
        core_copy(b).wait_send()
        x_copy(b).wait_send()
        return carry

    def drain_batch(n, carry):
        y_copy(n).wait_send()
        gy_copy(n).wait_send()
        gx_copy(n).wait_send()
        dx_copy(n).wait_send()
        dy_copy(n).wait_send()
        for i in range(4):
            c_copy(n, mine, i).wait_send()
        return carry

    lax.fori_loop(0, N_SEQ, drain_seq, 0)
    lax.fori_loop(0, N_BATCH, drain_batch, 0)


def block(q, k_new, v_new, resid, w_o, k_cache, v_cache, limits):
    rows = k_cache.shape[1] * 4
    vmem = pl.BlockSpec(memory_space=pltpu.VMEM)
    hbm = pl.BlockSpec(memory_space=pl.ANY)
    dma = pltpu.SemaphoreType.DMA
    return pl.pallas_call(
        block_kernel,
        out_shape=jax.ShapeDtypeStruct((N_SEQ, 32, 2048), jnp.bfloat16),
        in_specs=[pl.BlockSpec(memory_space=pltpu.SMEM), vmem, vmem, vmem, vmem, vmem, hbm, hbm],
        out_specs=vmem,
        scratch_shapes=[
            pltpu.VMEM((NBUF, rows, 128), jnp.bfloat16),
            pltpu.VMEM((NBUF, rows, 128), jnp.bfloat16),
            pltpu.VMEM((2, 2, 2048, 128), jnp.float32),
            pltpu.VMEM((2, 2, 32, 128), jnp.float32),
            pltpu.VMEM((2, 2, 8, 128), jnp.float32),
            pltpu.VMEM((N_SEQ, 32, 1152), jnp.float32),
            pltpu.VMEM((N_SEQ, 16, 1152), jnp.float32),
            pltpu.VMEM((N_SEQ, 16, 1152), jnp.float32),
            pltpu.VMEM((N_SEQ, 8, 1152), jnp.float32),
            pltpu.VMEM((N_BATCH, 2, BATCH * 8, 1024), jnp.float32),
            pltpu.VMEM((N_BATCH, BATCH * 8, 1024), jnp.float32),
            pltpu.VMEM((8, N_BATCH, BATCH * 8, 1024), jnp.float32),
            dma((NBUF,)), dma((NBUF,)),
            dma((N_SEQ,)), dma((N_SEQ,)), dma((N_SEQ,)), dma((N_SEQ,)),
            dma((N_BATCH,)), dma((N_BATCH,)), dma((N_BATCH,)), dma((N_BATCH,)), dma((N_BATCH,)), dma((N_BATCH,)),
            dma((N_BATCH,)), dma((N_BATCH,)), dma((N_BATCH,)), dma((N_BATCH,)), dma((4, N_BATCH)), dma((4, N_BATCH)),
        ],
        compiler_params=pltpu.CompilerParams(vmem_limit_bytes=62 * 1024 * 1024, collective_id=0, has_side_effects=True),
        cost_estimate=pl.CostEstimate(flops=19_000_000_000, bytes_accessed=140_000_000, transcendentals=17_000_000),
    )(limits, q, k_new.reshape(N_SEQ, 128, 128), v_new.reshape(N_SEQ, 128, 128), resid, w_o, k_cache.reshape(N_SEQ, rows, 128), v_cache.reshape(N_SEQ, rows, 128))


def solution(mesh):
    def per_device(hidden, prefix_len, k_cache, v_cache, attn_norm, w_q, w_k, w_v, w_o, q_norm, k_norm):
        cp = lax.axis_index('cp')
        tp = lax.axis_index('tp')
        q_rot, k_new, v_new = project_new(hidden, attn_norm, w_q, w_k, w_v, q_norm, k_norm, prefix_len)
        limits = jnp.concatenate([prefix_len - cp * 2048, jnp.where(cp == 3, 0, 64)[None]]).astype(jnp.int32)
        first = (cp % 2) * 16 + (cp // 2) * 8
        resid = lax.dynamic_slice(hidden, (0, first, tp * 1024), (N_SEQ, 8, 1024))
        block_out = block(q_rot.reshape(N_SEQ, 32, 1024), k_new, v_new, resid, w_o, k_cache, v_cache, limits)
        return block_out, k_new, v_new

    cache_spec = P('dp', 'cp', 'tp', None)
    arg_specs = (P('dp', None, None), P('dp'), cache_spec, cache_spec, P(None), P(None, 'tp'), P(None, 'tp'), P(None, 'tp'), P('tp', None), P(None), P(None))
    out_specs = (P('dp', None, None), P('dp', None, 'tp', None), P('dp', None, 'tp', None))
    return jax.shard_map(per_device, mesh=mesh, in_specs=arg_specs, out_specs=out_specs, check_vma=False)
```

```python
import jax
import jax.numpy as jnp
import numpy as np
from jax import lax
from jax.experimental import pallas as pl
from jax.experimental.pallas import tpu as pltpu
from jax.sharding import PartitionSpec as P

HEAD_DIM = 128
NEG = -3e38
FLOOR = -1e38
LOG2E = 1.4426950408889634
NBUF = 3
CHUNK = 256
SCALE = HEAD_DIM ** -0.5 * LOG2E


def rope_tables(prefix_len):
    inv_freq = 1e6 ** -(np.arange(HEAD_DIM) % 64 / 64.0)
    token_angles = np.arange(32)[:, None] * inv_freq
    off = np.concatenate([np.cos(token_angles), np.sin(token_angles)], axis=1).astype(np.float32)
    angles = prefix_len.astype(jnp.float32)[:, None] * inv_freq.astype(np.float32)
    return jnp.concatenate([jnp.cos(angles), jnp.sin(angles)], axis=1), jnp.asarray(off)


def project_kernel(x_ref, gain_ref, wq_ref, wk_ref, wv_ref, qn_ref, kn_ref, base_ref, off_ref, q_out, k_out, v_out, normed, kf, vf, cos_t, sin_t):
    i = pl.program_id(0)

    @pl.when(i == 0)
    def _():
        gain = gain_ref[...].astype(jnp.float32)

        def norm(m, carry):
            rows = pl.ds(pl.multiple_of(m * 128, 128), 128)
            t = x_ref[rows, :].astype(jnp.float32)
            normed[rows, :] = (t * lax.rsqrt(jnp.mean(t * t, axis=1, keepdims=True) + 1e-6) * gain).astype(jnp.bfloat16)
            return carry

        lax.fori_loop(0, 8, norm, 0)
        cb, sb = off_ref[:, :128], off_ref[:, 128:]
        lane = lax.broadcasted_iota(jnp.int32, (32, 128), 1)
        for b in range(32):
            ca, sa = base_ref[b:b + 1, :128], base_ref[b:b + 1, 128:]
            sin = sa * cb + ca * sb
            cos_t[b * 32:(b + 1) * 32, :] = ca * cb - sa * sb
            sin_t[b * 32:(b + 1) * 32, :] = jnp.where(lane < 64, -sin, sin)

    def head(lin, gain, rows):
        t = lin.astype(jnp.bfloat16).astype(jnp.float32)
        t = t * lax.rsqrt(jnp.mean(t * t, axis=1, keepdims=True) + 1e-6) * gain
        return (t * cos_t[rows, :] + pltpu.roll(t, 64, 1) * sin_t[rows, :]).astype(jnp.bfloat16)

    qg = qn_ref[...].astype(jnp.float32)
    kg = kn_ref[...].astype(jnp.float32)
    wkv = jnp.concatenate([wk_ref[...], wv_ref[...]], axis=1)
    for m in range(4):
        rows = slice(m * 256, (m + 1) * 256)
        q = jnp.dot(normed[rows, :], wq_ref[...], preferred_element_type=jnp.float32)
        kv = jnp.dot(normed[rows, :], wkv, preferred_element_type=jnp.float32)
        for g in range(2):
            q_out[rows, g * 128:(g + 1) * 128] = head(q[:, g * 128:(g + 1) * 128], qg, rows)
        spread = pl.ds(m * 1024 + i, 256, stride=4)
        kf[spread, :] = head(kv[:, :128], kg, rows).astype(jnp.float32)
        vf[spread, :] = kv[:, 128:]

    @pl.when(i == 3)
    def _():
        def finish(m, carry):
            rows = pl.ds(pl.multiple_of(m * 512, 512), 512)
            k_out[rows, :] = kf[rows, :].astype(jnp.bfloat16)
            v_out[rows, :] = vf[rows, :].astype(jnp.bfloat16)
            return carry

        lax.fori_loop(0, 8, finish, 0)


def project(hidden, attn_norm, w_q, w_k, w_v, q_norm, k_norm, prefix_len):
    base, off = rope_tables(prefix_len)
    whole = lambda shape: pl.BlockSpec(shape, lambda i: (0, 0))
    cols = lambda n, w: pl.BlockSpec((n, w), lambda i: (0, i))
    return pl.pallas_call(
        project_kernel,
        grid=(4,),
        out_shape=(jax.ShapeDtypeStruct((1024, 1024), jnp.bfloat16), jax.ShapeDtypeStruct((4096, 128), jnp.bfloat16), jax.ShapeDtypeStruct((4096, 128), jnp.bfloat16)),
        in_specs=[whole((1024, 2048)), whole((1, 2048)), cols(2048, 256), cols(2048, 128), cols(2048, 128), whole((1, 128)), whole((1, 128)), whole((32, 256)), whole((32, 256))],
        out_specs=(cols(1024, 256), whole((4096, 128)), whole((4096, 128))),
        scratch_shapes=[
            pltpu.VMEM((1024, 2048), jnp.bfloat16),
            pltpu.VMEM((4096, 128), jnp.float32),
            pltpu.VMEM((4096, 128), jnp.float32),
            pltpu.VMEM((1024, 128), jnp.float32),
            pltpu.VMEM((1024, 128), jnp.float32),
        ],
        compiler_params=pltpu.CompilerParams(vmem_limit_bytes=40 * 1024 * 1024),
        cost_estimate=pl.CostEstimate(flops=8_600_000_000, bytes_accessed=16_000_000, transcendentals=20_000),
    )(hidden.reshape(1024, 2048), attn_norm.reshape(1, 2048), w_q, w_k, w_v, q_norm.reshape(1, 128), k_norm.reshape(1, 128), base, off)


def head_rows(ref, start, count, head):
    return ref[pl.ds(start * 4 + head, count, stride=4), :]


def pair_rows(ref, start, count, pair):
    return jnp.concatenate([head_rows(ref, start, count, 2 * pair), head_rows(ref, start, count, 2 * pair + 1)], axis=1)


def query_weights(q_ref, b, pair):
    def head(h):
        return jnp.concatenate([q_ref[b, :, (2 * h + g) * 128:(2 * h + g + 1) * 128] for g in range(2)], axis=0)
    zero = jnp.zeros((64, 128), jnp.bfloat16)
    top = jnp.concatenate([head(2 * pair), zero], axis=1)
    low = jnp.concatenate([zero, head(2 * pair + 1)], axis=1)
    return jnp.concatenate([top, low], axis=0).T


def masked_scores(keys, wq, mask):
    return jnp.where(mask, jnp.dot(keys, wq, preferred_element_type=jnp.float32), NEG)


def fold_rows(op, tensor):
    return op(tensor.reshape(tensor.shape[0] // 8, 8, 128), axis=0)


def attend_step(q_ref, kn_ref, vn_ref, kbuf, vbuf, scores, own_scores, tops, b, nxt, limit, own):
    row = lax.broadcasted_iota(jnp.int32, (CHUNK, 128), 0)
    wq = [query_weights(q_ref, nxt, pair) for pair in range(2)]
    new_top = [jnp.full((8, 128), FLOOR, jnp.float32) for _ in range(2)]
    total = [jnp.zeros((8, 128), jnp.float32) for _ in range(2)]
    out = [jnp.zeros((128, 256), jnp.float32) for _ in range(2)]

    def values(pair, s, vals):
        p = jnp.exp2((s - tops[pair]) * SCALE)
        total[pair] = total[pair] + fold_rows(jnp.sum, p)
        out[pair] = out[pair] + jnp.dot(p.astype(jnp.bfloat16).T, vals, preferred_element_type=jnp.float32)

    for c in range(2048 // CHUNK):
        rows = pl.ds(c * CHUNK, CHUNK)
        mask = row < limit - c * CHUNK
        for pair in range(2):
            if tops is not None:
                values(pair, scores[pair, rows, :], pair_rows(vbuf, c * CHUNK, CHUNK, pair))
            s = masked_scores(pair_rows(kbuf, c * CHUNK, CHUNK, pair), wq[pair], mask)
            scores[pair, rows, :] = s
            new_top[pair] = jnp.maximum(new_top[pair], fold_rows(jnp.max, s))
    token = lax.broadcasted_iota(jnp.int32, (32, 128), 1) % 32
    mask = lax.broadcasted_iota(jnp.int32, (32, 128), 0) <= token - own
    for pair in range(2):
        if tops is not None:
            values(pair, own_scores[pair], pair_rows(vn_ref.at[b], 0, 32, pair))
        s = masked_scores(pair_rows(kn_ref.at[nxt], 0, 32, pair), wq[pair], mask)
        own_scores[pair] = s
        new_top[pair] = jnp.maximum(new_top[pair], fold_rows(jnp.max, s))
    return out, [jnp.sum(t, axis=0, keepdims=True) for t in total], [jnp.max(t, axis=0, keepdims=True) for t in new_top]


def stat_tile(rows, lane0):
    lane = lax.broadcasted_iota(jnp.int32, (32, 128), 1)
    tile = jnp.zeros((32, 128), jnp.float32)
    for pair in range(2):
        col = jnp.broadcast_to(rows[pair], (128, 128)).T
        for i in range(4):
            tile = jnp.where(lane == lane0 + 4 * pair + i, col[i * 32:(i + 1) * 32], tile)
    return tile


N_SEQ = 32
BATCH = 4
N_BATCH = N_SEQ // BATCH
LAG_X, LAG_Y, LAG_G, LAG_D, LAG_F = 6, 9, 13, 16, 18
MESH = pl.DeviceIdType.MESH


def merge_parts(a, r):
    sa, sr = a[:, 1024:], r[:, 1024:]
    lane = lax.broadcasted_iota(jnp.int32, sa.shape, 1)
    top = jnp.maximum(sa, sr)
    fa = jnp.where(lane < 8, jnp.exp2((sa - top) * SCALE), 0.0)
    fr = jnp.where(lane < 8, jnp.exp2((sr - top) * SCALE), 0.0)
    total = sa * pltpu.roll(fa, 8, 1) + sr * pltpu.roll(fr, 8, 1)
    parts = []
    for h in range(8):
        cols = slice(h * 128, (h + 1) * 128)
        parts.append(a[:, cols] * fa[:, h:h + 1] + r[:, cols] * fr[:, h:h + 1])
    return parts, jnp.where(lane < 8, top, total)


def block_kernel(prefix_ref, q_ref, kn_ref, vn_ref, wo_ref, x_hbm, k_hbm, v_hbm, out_ref,
                 kbuf, vbuf, scores, own_scores, tops_ref, x_ref, part, part_in, half, half_in, proj, proj_in, gath,
                 ksem, vsem, xsem, d_send, d_recv, x_send, x_recv, y_send, y_recv, gx_send, gx_recv, gy_send, gy_recv,
                 dx_send, dx_recv, dy_send, dy_recv, c_send, c_recv):
    dp, tp, cp = lax.axis_index('dp'), lax.axis_index('tp'), lax.axis_index('cp')
    x, k = cp // 2, cp % 2
    core_peer = (dp, tp, cp + 1 - 2 * k)
    x_peer = (dp, tp, cp + 2 - 4 * x)
    y_peer = (dp, 1 - tp, cp)

    barrier = pltpu.get_barrier_semaphore()
    for peer in (core_peer, x_peer, y_peer):
        pl.semaphore_signal(barrier, inc=1, device_id=peer, device_id_type=MESH)

    def copies(b):
        slot = lax.rem(b, NBUF)
        return (pltpu.make_async_copy(k_hbm.at[b], kbuf.at[slot], ksem.at[slot]),
                pltpu.make_async_copy(v_hbm.at[b], vbuf.at[slot], vsem.at[slot]))

    def remote(src, dst, send, recv, peer):
        return pltpu.make_async_remote_copy(src_ref=src, dst_ref=dst, send_sem=send, recv_sem=recv, device_id=peer, device_id_type=MESH)

    def core_copy(b):
        return remote(part.at[b, pl.ds(pl.multiple_of((1 - k) * 16, 16), 16)], part_in.at[b], d_send.at[b], d_recv.at[b], core_peer)

    def x_copy(b):
        return remote(half.at[b, pl.ds(pl.multiple_of((1 - x) * 8, 8), 8)], half_in.at[b], x_send.at[b], x_recv.at[b], x_peer)

    def y_copy(n):
        return remote(proj.at[n, 1 - tp], proj_in.at[n], y_send.at[n], y_recv.at[n], y_peer)

    def slot_of(xx, yy, kk):
        return (xx * 2 + yy) * 2 + kk

    mine = slot_of(x, tp, k)
    from_x = slot_of(1 - x, tp, k)
    from_y = slot_of(x, 1 - tp, k)
    diag = slot_of(1 - x, 1 - tp, k)

    def gx_copy(n):
        return remote(gath.at[mine, n], gath.at[mine, n], gx_send.at[n], gx_recv.at[n], x_peer)

    def gy_copy(n):
        return remote(gath.at[mine, n], gath.at[mine, n], gy_send.at[n], gy_recv.at[n], y_peer)

    def dx_copy(n):
        return remote(gath.at[from_y, n, pl.ds(0, 16)], gath.at[from_y, n, pl.ds(0, 16)], dx_send.at[n], dx_recv.at[n], x_peer)

    def dy_copy(n):
        return remote(gath.at[from_x, n, pl.ds(16, 16)], gath.at[from_x, n, pl.ds(16, 16)], dy_send.at[n], dy_recv.at[n], y_peer)

    def c_copy(n, slot, i):
        return remote(gath.at[slot, n], gath.at[slot, n], c_send.at[i, n], c_recv.at[i, n], core_peer)

    for b in range(NBUF - 1):
        for copy in copies(b):
            copy.start()
    own = jnp.where(cp == 3, 0, 64)

    first = k * 16 + x * 8
    x_load = pltpu.make_async_copy(x_hbm.at[:, pl.ds(pl.multiple_of(first, 8), 8), pl.ds(pl.multiple_of(tp * 1024, 1024), 1024)], x_ref, xsem)
    x_load.start()

    def limit_of(b):
        return prefix_ref[b] - cp * 2048

    def keep_tops(tops):
        for pair in range(2):
            tops_ref[pair] = jnp.broadcast_to(tops[pair], (8, 128))

    copies(0)[0].wait()
    keep_tops(attend_step(q_ref, kn_ref, vn_ref, kbuf.at[0], None, scores, own_scores, None, 0, 0, limit_of(0), own)[2])
    pl.semaphore_wait(barrier, 3)
    x_load.wait()

    def step(it, carry):
        @pl.when(it < N_SEQ)
        def _():
            b = it
            nxt = jnp.minimum(b + 1, N_SEQ - 1)
            copies(b)[1].wait()

            @pl.when(b + 1 < N_SEQ)
            def _():
                copies(b + 1)[0].wait()

            @pl.when(b + NBUF - 1 < N_SEQ)
            def _():
                for copy in copies(b + NBUF - 1):
                    copy.start()

            tops = [tops_ref[pair, 0:1, :] for pair in range(2)]
            outs, sums, new_tops = attend_step(q_ref, kn_ref, vn_ref, kbuf.at[lax.rem(nxt, NBUF)], vbuf.at[lax.rem(b, NBUF)], scores, own_scores,
                                               tops, b, nxt, limit_of(nxt), own)
            keep_tops(new_tops)
            for pair in range(2):
                out = outs[pair]
                for i in range(4):
                    head = 4 * pair + i
                    part[b, :, head * 128:(head + 1) * 128] = out[i * 32:(i + 1) * 32, (i // 2) * 128:(i // 2 + 1) * 128]
            part[b, :, 1024:1152] = stat_tile(tops, 0) + stat_tile(sums, 8)
            core_copy(b).start()

        @pl.when((it >= 1) & (it < N_SEQ + 1))
        def _():
            b = it - 1
            core_copy(b).wait_recv()
            parts, stats = merge_parts(part[b, pl.ds(pl.multiple_of(k * 16, 16), 16), :], part_in[b])
            for h in range(8):
                half[b, :, h * 128:(h + 1) * 128] = parts[h]
            half[b, :, 1024:] = stats
            x_copy(b).start()

        def batch_of(lag):
            n = (it - lag) // BATCH
            return n, (it >= lag) & ((it - lag) % BATCH == 0) & (n < N_BATCH)

        n_x, now_x = batch_of(LAG_X)

        @pl.when(now_x)
        def _():
            n = n_x
            for i in range(BATCH):
                x_copy(n * BATCH + i).wait_recv()
            seqs = pl.ds(n * BATCH, BATCH)
            a = half[seqs, pl.ds(pl.multiple_of(x * 8, 8), 8), :].reshape(BATCH * 8, 1152)
            r = half_in[seqs].reshape(BATCH * 8, 1152)
            parts, stats = merge_parts(a, r)
            inv = 1.0 / stats[:, 8:16]
            o = jnp.concatenate([parts[h] * inv[:, h:h + 1] for h in range(8)], axis=1).astype(jnp.bfloat16)
            for y in range(2):
                proj[n, y] = jnp.dot(o, wo_ref[:, y * 1024:(y + 1) * 1024], preferred_element_type=jnp.float32)
            y_copy(n).start()

        n_y, now_y = batch_of(LAG_Y)

        @pl.when(now_y)
        def _():
            n = n_y
            y_copy(n).wait_recv()
            res = x_ref[pl.ds(n * BATCH, BATCH)].reshape(BATCH * 8, 1024).astype(jnp.float32)
            gath[mine, n] = proj[n, tp] + proj_in[n] + res
            gy_copy(n).start()
            gx_copy(n).start()
            c_copy(n, mine, 0).start()

        n_g, now_g = batch_of(LAG_G)

        @pl.when(now_g)
        def _():
            n = n_g
            gy_copy(n).wait_recv()
            dx_copy(n).start()
            c_copy(n, from_y, 1).start()
            gx_copy(n).wait_recv()
            dy_copy(n).start()
            c_copy(n, from_x, 2).start()

        n_d, now_d = batch_of(LAG_D)

        @pl.when(now_d)
        def _():
            n = n_d
            dx_copy(n).wait_recv()
            dy_copy(n).wait_recv()
            c_copy(n, diag, 3).start()

        n_f, now_f = batch_of(LAG_F)

        @pl.when(now_f)
        def _():
            n = n_f
            for i in range(4):
                c_copy(n, mine, i).wait_recv()
            for kk in range(2):
                for y in range(2):
                    lo = gath[slot_of(0, y, kk), n].reshape(BATCH, 8, 1024)
                    hi = gath[slot_of(1, y, kk), n].reshape(BATCH, 8, 1024)
                    out_ref[pl.ds(n * BATCH, BATCH), kk * 16:(kk + 1) * 16, y * 1024:(y + 1) * 1024] = jnp.concatenate([lo, hi], axis=1).astype(jnp.bfloat16)

        return carry

    lax.fori_loop(0, N_SEQ + LAG_F - BATCH + 1, step, 0)

    def drain_seq(b, carry):
        core_copy(b).wait_send()
        x_copy(b).wait_send()
        return carry

    def drain_batch(n, carry):
        y_copy(n).wait_send()
        gy_copy(n).wait_send()
        gx_copy(n).wait_send()
        dx_copy(n).wait_send()
        dy_copy(n).wait_send()
        for i in range(4):
            c_copy(n, mine, i).wait_send()
        return carry

    lax.fori_loop(0, N_SEQ, drain_seq, 0)
    lax.fori_loop(0, N_BATCH, drain_batch, 0)


def block(q, k_rows, v_rows, hidden, w_o, k_cache, v_cache, prefix_len):
    rows = k_cache.shape[1] * 4
    vmem = pl.BlockSpec(memory_space=pltpu.VMEM)
    hbm = pl.BlockSpec(memory_space=pl.ANY)
    dma = pltpu.SemaphoreType.DMA
    return pl.pallas_call(
        block_kernel,
        out_shape=jax.ShapeDtypeStruct((N_SEQ, 32, 2048), jnp.bfloat16),
        in_specs=[pl.BlockSpec(memory_space=pltpu.SMEM), vmem, vmem, vmem, vmem, hbm, hbm, hbm],
        out_specs=vmem,
        scratch_shapes=[
            pltpu.VMEM((NBUF, rows, 128), jnp.bfloat16),
            pltpu.VMEM((NBUF, rows, 128), jnp.bfloat16),
            pltpu.VMEM((2, 2048, 128), jnp.float32),
            pltpu.VMEM((2, 32, 128), jnp.float32),
            pltpu.VMEM((2, 8, 128), jnp.float32),
            pltpu.VMEM((N_SEQ, 8, 1024), jnp.bfloat16),
            pltpu.VMEM((N_SEQ, 32, 1152), jnp.float32),
            pltpu.VMEM((N_SEQ, 16, 1152), jnp.float32),
            pltpu.VMEM((N_SEQ, 16, 1152), jnp.float32),
            pltpu.VMEM((N_SEQ, 8, 1152), jnp.float32),
            pltpu.VMEM((N_BATCH, 2, BATCH * 8, 1024), jnp.float32),
            pltpu.VMEM((N_BATCH, BATCH * 8, 1024), jnp.float32),
            pltpu.VMEM((8, N_BATCH, BATCH * 8, 1024), jnp.float32),
            dma((NBUF,)), dma((NBUF,)), dma,
            dma((N_SEQ,)), dma((N_SEQ,)), dma((N_SEQ,)), dma((N_SEQ,)),
            dma((N_BATCH,)), dma((N_BATCH,)), dma((N_BATCH,)), dma((N_BATCH,)), dma((N_BATCH,)), dma((N_BATCH,)),
            dma((N_BATCH,)), dma((N_BATCH,)), dma((N_BATCH,)), dma((N_BATCH,)), dma((4, N_BATCH)), dma((4, N_BATCH)),
        ],
        compiler_params=pltpu.CompilerParams(vmem_limit_bytes=62 * 1024 * 1024, collective_id=0, has_side_effects=True),
        cost_estimate=pl.CostEstimate(flops=19_000_000_000, bytes_accessed=140_000_000, transcendentals=17_000_000),
    )(prefix_len, q, k_rows, v_rows, w_o, hidden, k_cache.reshape(N_SEQ, rows, 128), v_cache.reshape(N_SEQ, rows, 128))


def solution(mesh):
    def per_device(hidden, prefix_len, k_cache, v_cache, attn_norm, w_q, w_k, w_v, w_o, q_norm, k_norm):
        q, k_rows, v_rows = project(hidden, attn_norm, w_q, w_k, w_v, q_norm, k_norm, prefix_len)
        block_out = block(q.reshape(N_SEQ, 32, 1024), k_rows.reshape(N_SEQ, 128, 128), v_rows.reshape(N_SEQ, 128, 128), hidden, w_o, k_cache, v_cache, prefix_len)
        return block_out, k_rows.reshape(N_SEQ, 32, 4, 128), v_rows.reshape(N_SEQ, 32, 4, 128)

    cache_spec = P('dp', 'cp', 'tp', None)
    arg_specs = (P('dp', None, None), P('dp'), cache_spec, cache_spec, P(None), P(None, 'tp'), P(None, 'tp'), P(None, 'tp'), P('tp', None), P(None), P(None))
    out_specs = (P('dp', None, None), P('dp', None, 'tp', None), P('dp', None, 'tp', None))
    return jax.shard_map(per_device, mesh=mesh, in_specs=arg_specs, out_specs=out_specs, check_vma=False)
```

```python
import jax
import jax.numpy as jnp
import numpy as np
from jax import lax
from jax.experimental import pallas as pl
from jax.experimental.pallas import tpu as pltpu
from jax.sharding import PartitionSpec as P

HEAD_DIM = 128
NEG = -3e38
FLOOR = -1e38
LOG2E = 1.4426950408889634
NBUF = 4
CHUNK = 256
SCALE = HEAD_DIM ** -0.5 * LOG2E


def rope_tables(prefix_len):
    freq = (1.0 / 1e6 ** (np.arange(HEAD_DIM) % 64 / 64.0)).astype(np.float32)
    token_angles = np.arange(32, dtype=np.float32)[:, None] * freq
    wide = token_angles.astype(np.float64)
    off = np.concatenate([np.cos(wide), np.sin(wide)], axis=1).astype(np.float32)
    angles = prefix_len.astype(jnp.float32)[:, None] * freq
    return jnp.concatenate([jnp.cos(angles), jnp.sin(angles)], axis=1), jnp.asarray(off), jnp.asarray(freq[None])


def project_kernel(x_ref, gain_ref, wq_ref, wk_ref, wv_ref, qn_ref, kn_ref, base_ref, off_ref, freq_ref, prefix_ref, q_out, k_out, v_out, normed, kf, vf, cos_t, sin_t):
    i = pl.program_id(0)

    @pl.when(i == 0)
    def _():
        gain = gain_ref[...].astype(jnp.float32)

        def norm(m, carry):
            rows = pl.ds(pl.multiple_of(m * 128, 128), 128)
            t = x_ref[rows, :].astype(jnp.float32)
            normed[rows, :] = (t * lax.rsqrt(jnp.mean(t * t, axis=1, keepdims=True) + 1e-6) * gain).astype(jnp.bfloat16)
            return carry

        lax.fori_loop(0, 8, norm, 0)
        cb, sb = off_ref[:, :128], off_ref[:, 128:]
        freq = freq_ref[...]
        lane = lax.broadcasted_iota(jnp.int32, (32, 128), 1)
        token = lax.broadcasted_iota(jnp.int32, (32, 128), 0)
        token_angle = token.astype(jnp.float32) * freq
        for b in range(32):
            ca, sa = base_ref[b:b + 1, :128], base_ref[b:b + 1, 128:]
            prefix = prefix_ref[b]
            angle = (token + prefix).astype(jnp.float32) * freq
            base_angle = jnp.full((1, 128), prefix, jnp.int32).astype(jnp.float32) * freq
            eps = (angle - base_angle) - token_angle
            near = 1.0 - 0.5 * eps * eps
            ct, st = cb * near - sb * eps, sb * near + cb * eps
            sin = sa * ct + ca * st
            cos_t[b * 32:(b + 1) * 32, :] = ca * ct - sa * st
            sin_t[b * 32:(b + 1) * 32, :] = jnp.where(lane < 64, -sin, sin)

    def head(lin, gain, rows):
        t = lin.astype(jnp.bfloat16).astype(jnp.float32)
        t = t * lax.rsqrt(jnp.mean(t * t, axis=1, keepdims=True) + 1e-6) * gain
        return (t * cos_t[rows, :] + pltpu.roll(t, 64, 1) * sin_t[rows, :]).astype(jnp.bfloat16)

    qg = qn_ref[...].astype(jnp.float32)
    kg = kn_ref[...].astype(jnp.float32)
    wkv = jnp.concatenate([wk_ref[...], wv_ref[...]], axis=1)
    for m in range(4):
        rows = slice(m * 256, (m + 1) * 256)
        q = jnp.dot(normed[rows, :], wq_ref[...], preferred_element_type=jnp.float32)
        kv = jnp.dot(normed[rows, :], wkv, preferred_element_type=jnp.float32)
        for g in range(2):
            q_out[rows, g * 128:(g + 1) * 128] = head(q[:, g * 128:(g + 1) * 128], qg, rows)
        spread = pl.ds(m * 1024 + i, 256, stride=4)
        kf[spread, :] = head(kv[:, :128], kg, rows).astype(jnp.float32)
        vf[spread, :] = kv[:, 128:]

    @pl.when(i == 3)
    def _():
        def finish(m, carry):
            rows = pl.ds(pl.multiple_of(m * 512, 512), 512)
            k_out[rows, :] = kf[rows, :].astype(jnp.bfloat16)
            v_out[rows, :] = vf[rows, :].astype(jnp.bfloat16)
            return carry

        lax.fori_loop(0, 8, finish, 0)


def project(hidden, attn_norm, w_q, w_k, w_v, q_norm, k_norm, prefix_len):
    base, off, freq = rope_tables(prefix_len)
    whole = lambda shape: pl.BlockSpec(shape, lambda i: (0, 0))
    cols = lambda n, w: pl.BlockSpec((n, w), lambda i: (0, i))
    return pl.pallas_call(
        project_kernel,
        grid=(4,),
        out_shape=(jax.ShapeDtypeStruct((1024, 1024), jnp.bfloat16), jax.ShapeDtypeStruct((4096, 128), jnp.bfloat16), jax.ShapeDtypeStruct((4096, 128), jnp.bfloat16)),
        in_specs=[whole((1024, 2048)), whole((1, 2048)), cols(2048, 256), cols(2048, 128), cols(2048, 128), whole((1, 128)), whole((1, 128)), whole((32, 256)), whole((32, 256)), whole((1, 128)), pl.BlockSpec(memory_space=pltpu.SMEM)],
        out_specs=(cols(1024, 256), whole((4096, 128)), whole((4096, 128))),
        scratch_shapes=[
            pltpu.VMEM((1024, 2048), jnp.bfloat16),
            pltpu.VMEM((4096, 128), jnp.float32),
            pltpu.VMEM((4096, 128), jnp.float32),
            pltpu.VMEM((1024, 128), jnp.float32),
            pltpu.VMEM((1024, 128), jnp.float32),
        ],
        compiler_params=pltpu.CompilerParams(vmem_limit_bytes=62 * 1024 * 1024),
        cost_estimate=pl.CostEstimate(flops=8_600_000_000, bytes_accessed=16_000_000, transcendentals=20_000),
    )(hidden.reshape(1024, 2048), attn_norm.reshape(1, 2048), w_q, w_k, w_v, q_norm.reshape(1, 128), k_norm.reshape(1, 128), base, off, freq, prefix_len)


def head_rows(ref, start, count, head):
    return ref[pl.ds(start * 4 + head, count, stride=4), :]


def pair_rows(ref, start, count, pair):
    return jnp.concatenate([head_rows(ref, start, count, 2 * pair), head_rows(ref, start, count, 2 * pair + 1)], axis=1)


def query_weights(q_ref, b, pair):
    def head(h):
        return jnp.concatenate([q_ref[b, :, (2 * h + g) * 128:(2 * h + g + 1) * 128] for g in range(2)], axis=0)
    zero = jnp.zeros((64, 128), jnp.bfloat16)
    top = jnp.concatenate([head(2 * pair), zero], axis=1)
    low = jnp.concatenate([zero, head(2 * pair + 1)], axis=1)
    return jnp.concatenate([top, low], axis=0).T


def masked_scores(keys, wq, mask):
    return jnp.where(mask, jnp.dot(keys, wq, preferred_element_type=jnp.float32), NEG)


def fold_rows(op, tensor):
    return op(tensor.reshape(tensor.shape[0] // 8, 8, 128), axis=0)


def attend_step(q_ref, kn_ref, vn_ref, kbuf, vbuf, scores, own_scores, tops, b, nxt, limit, own, between=()):
    row = lax.broadcasted_iota(jnp.int32, (CHUNK, 128), 0)
    wq = [query_weights(q_ref, nxt, pair) for pair in range(2)]
    new_top = [jnp.full((8, 128), FLOOR, jnp.float32) for _ in range(2)]
    total = [jnp.zeros((8, 128), jnp.float32) for _ in range(2)]
    out = [jnp.zeros((128, 256), jnp.float32) for _ in range(2)]

    def values(pair, s, vals):
        p = jnp.exp2((s - tops[pair]) * SCALE)
        total[pair] = total[pair] + fold_rows(jnp.sum, p)
        out[pair] = out[pair] + jnp.dot(p.astype(jnp.bfloat16).T, vals, preferred_element_type=jnp.float32)

    for c in range(2048 // CHUNK):
        rows = pl.ds(c * CHUNK, CHUNK)
        mask = row < limit - c * CHUNK
        for pair in range(2):
            if tops is not None:
                values(pair, scores[pair, rows, :], pair_rows(vbuf, c * CHUNK, CHUNK, pair))
            s = masked_scores(pair_rows(kbuf, c * CHUNK, CHUNK, pair), wq[pair], mask)
            scores[pair, rows, :] = s
            new_top[pair] = jnp.maximum(new_top[pair], fold_rows(jnp.max, s))
        for work in between[c::2048 // CHUNK]:
            work()
    token = lax.broadcasted_iota(jnp.int32, (32, 128), 1) % 32
    mask = lax.broadcasted_iota(jnp.int32, (32, 128), 0) <= token - own
    for pair in range(2):
        if tops is not None:
            values(pair, own_scores[pair], pair_rows(vn_ref.at[b], 0, 32, pair))
        s = masked_scores(pair_rows(kn_ref.at[nxt], 0, 32, pair), wq[pair], mask)
        own_scores[pair] = s
        new_top[pair] = jnp.maximum(new_top[pair], fold_rows(jnp.max, s))
    return out, [jnp.sum(t, axis=0, keepdims=True) for t in total], [jnp.max(t, axis=0, keepdims=True) for t in new_top]


def stat_tile(rows, lane0):
    lane = lax.broadcasted_iota(jnp.int32, (32, 128), 1)
    tile = jnp.zeros((32, 128), jnp.float32)
    for pair in range(2):
        col = jnp.broadcast_to(rows[pair], (128, 128)).T
        for i in range(4):
            tile = jnp.where(lane == lane0 + 4 * pair + i, col[i * 32:(i + 1) * 32], tile)
    return tile


N_SEQ = 32
BATCH = 2
N_BATCH = N_SEQ // BATCH
LAG_X, LAG_Y, LAG_G, LAG_D, LAG_F = 6, 9, 14, 18, 21
MESH = pl.DeviceIdType.MESH


def merge_parts(a, r):
    sa, sr = a[:, 1024:], r[:, 1024:]
    lane = lax.broadcasted_iota(jnp.int32, sa.shape, 1)
    top = jnp.maximum(sa, sr)
    fa = jnp.where(lane < 8, jnp.exp2((sa - top) * SCALE), 0.0)
    fr = jnp.where(lane < 8, jnp.exp2((sr - top) * SCALE), 0.0)
    total = sa * pltpu.roll(fa, 8, 1) + sr * pltpu.roll(fr, 8, 1)
    parts = []
    for h in range(8):
        cols = slice(h * 128, (h + 1) * 128)
        parts.append(a[:, cols] * fa[:, h:h + 1] + r[:, cols] * fr[:, h:h + 1])
    return parts, jnp.where(lane < 8, top, total)


def block_kernel(prefix_ref, q_ref, kn_ref, vn_ref, wo_hbm, x_hbm, k_hbm, v_hbm, out_ref,
                 kbuf, vbuf, scores, own_scores, tops_ref, x_ref, wo_ref, part, part_in, half, half_in, proj, proj_in, gath,
                 ksem, vsem, xsem, wsem, d_send, d_recv, x_send, x_recv, y_send, y_recv, gx_send, gx_recv, gy_send, gy_recv,
                 g_send, g_recv, c_send, c_recv):
    dp, tp, cp = lax.axis_index('dp'), lax.axis_index('tp'), lax.axis_index('cp')
    x, k = cp // 2, cp % 2
    core_peer = (dp, tp, cp + 1 - 2 * k)
    x_peer = (dp, tp, cp + 2 - 4 * x)
    y_peer = (dp, 1 - tp, cp)

    barrier = pltpu.get_barrier_semaphore()
    for peer in (core_peer, x_peer, y_peer):
        pl.semaphore_signal(barrier, inc=1, device_id=peer, device_id_type=MESH)

    def copies(b):
        slot = lax.rem(b, NBUF)
        return (pltpu.make_async_copy(k_hbm.at[b], kbuf.at[slot], ksem.at[slot]),
                pltpu.make_async_copy(v_hbm.at[b], vbuf.at[slot], vsem.at[slot]))

    def remote(src, dst, send, recv, peer):
        return pltpu.make_async_remote_copy(src_ref=src, dst_ref=dst, send_sem=send, recv_sem=recv, device_id=peer, device_id_type=MESH)

    def core_copy(b):
        return remote(part.at[b, pl.ds(pl.multiple_of((1 - k) * 16, 16), 16)], part_in.at[b], d_send.at[b], d_recv.at[b], core_peer)

    def x_copy(b):
        return remote(half.at[b, pl.ds(pl.multiple_of((1 - x) * 8, 8), 8)], half_in.at[b], x_send.at[b], x_recv.at[b], x_peer)

    def y_copy(n):
        return remote(proj.at[n, 1 - tp], proj_in.at[n], y_send.at[n], y_recv.at[n], y_peer)

    mine, from_x, from_y = x * 2 + tp, (1 - x) * 2 + tp, x * 2 + 1 - tp

    def gath_copy(s, slot, send, recv, peer):
        return remote(gath.at[s, k, slot], gath.at[s, k, slot], send.at[s], recv.at[s], peer)

    def gx_copy(s):
        return gath_copy(s, mine, gx_send, gx_recv, x_peer)

    def gy_copy(s):
        return gath_copy(s, mine, gy_send, gy_recv, y_peer)

    def diag_copy(s, odd):
        if odd:
            return gath_copy(s, from_x, g_send, g_recv, y_peer)
        return gath_copy(s, from_y, g_send, g_recv, x_peer)

    def c_copy(s):
        return remote(gath.at[s, k], gath.at[s, k], c_send.at[s], c_recv.at[s], core_peer)

    for b in range(NBUF - 1):
        for copy in copies(b):
            copy.start()
    own = jnp.where(cp == 3, 0, 64)

    first = k * 16 + x * 8
    x_load = pltpu.make_async_copy(x_hbm.at[:, pl.ds(pl.multiple_of(first, 8), 8), pl.ds(pl.multiple_of(tp * 1024, 1024), 1024)], x_ref, xsem)
    x_load.start()
    wo_load = pltpu.make_async_copy(wo_hbm, wo_ref, wsem)
    wo_load.start()

    def limit_of(b):
        return prefix_ref[b] - cp * 2048

    def keep_tops(tops):
        for pair in range(2):
            tops_ref[pair] = jnp.broadcast_to(tops[pair], (8, 128))

    copies(0)[0].wait()
    keep_tops(attend_step(q_ref, kn_ref, vn_ref, kbuf.at[0], None, scores, own_scores, None, 0, 0, limit_of(0), own)[2])
    pl.semaphore_wait(barrier, 3)
    x_load.wait()
    wo_load.wait()

    def merge_core(b):
        parts, stats = merge_parts(part[jnp.minimum(b, N_SEQ - 1), pl.ds(pl.multiple_of(k * 16, 16), 16), :], part_in[b])
        for h in range(8):
            half[b, :, h * 128:(h + 1) * 128] = parts[h]
        half[b, :, 1024:] = stats

    def wait_x(n):
        for i in range(BATCH):
            x_copy(n * BATCH + i).wait_recv()

    def normalized(n):
        seqs = pl.ds(n * BATCH, BATCH)
        a = half[seqs, pl.ds(pl.multiple_of(x * 8, 8), 8), :].reshape(BATCH * 8, 1152)
        r = half_in[seqs].reshape(BATCH * 8, 1152)
        parts, stats = merge_parts(a, r)
        inv = 1.0 / stats[:, 8:16]
        return jnp.concatenate([parts[h] * inv[:, h:h + 1] for h in range(8)], axis=1).astype(jnp.bfloat16)

    def project_part(n, o, y, q):
        lo = y * 1024 + q * 512
        proj[n, y, :, q * 512:(q + 1) * 512] = jnp.dot(o, wo_ref[:, lo:lo + 512], preferred_element_type=jnp.float32)

    def project_out(n):
        o = normalized(n)
        for y in range(2):
            for q in range(2):
                project_part(n, o, y, q)

    def add_peer(n):
        res = x_ref[pl.ds(jnp.minimum(n, N_BATCH - 1) * BATCH, BATCH)].reshape(BATCH * 8, 1024).astype(jnp.float32)
        gath[pl.ds(n * BATCH, BATCH), k, mine] = (proj[n, tp] + proj_in[n] + res).reshape(BATCH, 8, 1024)

    def send_mine(s):
        gy_copy(s).start()
        gx_copy(s).start()

    def forward(s, odd):
        gy_copy(s).wait_recv()
        gx_copy(s).wait_recv()
        diag_copy(s, odd).start()

    def forward_core(s, odd):
        diag_copy(s, odd).wait_recv()
        c_copy(s).start()

    def finish(s):
        at = jnp.minimum(s, N_SEQ - 1)
        for kk in range(2):
            for y in range(2):
                both = jnp.concatenate([gath[s, kk, y], gath[s, kk, 2 + y]], axis=0)
                out_ref[at, kk * 16:(kk + 1) * 16, y * 1024:(y + 1) * 1024] = both.astype(jnp.bfloat16)

    at_x, at_y = (divmod(lag, BATCH)[::-1] for lag in (LAG_X, LAG_Y))

    def batch_step(n, carry):
        def behind(at):
            return jnp.where(n >= at[1], n - at[1], N_BATCH)

        for j in range(BATCH):
            b = n * BATCH + j
            nxt = jnp.minimum(b + 1, N_SEQ - 1)

            def lagged(lag, b=b):
                return jnp.where(b >= lag, b - lag, N_SEQ)

            copies(b)[1].wait()

            @pl.when(b + 1 < N_SEQ)
            def _():
                copies(b + 1)[0].wait()

            @pl.when(b + NBUF - 1 < N_SEQ)
            def _():
                for copy in copies(b + NBUF - 1):
                    copy.start()

            @pl.when(b >= 2)
            def _():
                core_copy(b - 2).wait_recv()

            if at_x[0] == j:
                @pl.when(n >= at_x[1])
                def _():
                    wait_x(n - at_x[1])
            if at_y[0] == j:
                @pl.when(n >= at_y[1])
                def _():
                    y_copy(n - at_y[1]).wait_recv()

            @pl.when(b >= LAG_G)
            def _():
                forward(b - LAG_G, (j - LAG_G) % 2)

            @pl.when(b >= LAG_D)
            def _():
                forward_core(b - LAG_D, (j - LAG_D) % 2)

            @pl.when(b >= LAG_F)
            def _():
                c_copy(b - LAG_F).wait_recv()

            between = [lambda b=b: merge_core(lagged(2, b)), lambda b=b: finish(lagged(LAG_F, b))]
            if at_y[0] == j:
                between.append(lambda: add_peer(behind(at_y)))
            if at_x[0] == j:
                parts_of = normalized(behind(at_x))
                between += [lambda y=y, q=q: project_part(behind(at_x), parts_of, y, q) for y in range(2) for q in range(2)]
            tops = [tops_ref[pair, 0:1, :] for pair in range(2)]
            outs, sums, new_tops = attend_step(q_ref, kn_ref, vn_ref, kbuf.at[lax.rem(nxt, NBUF)], vbuf.at[lax.rem(b, NBUF)], scores, own_scores,
                                               tops, b, nxt, limit_of(nxt), own, between)
            keep_tops(new_tops)
            for pair in range(2):
                out = outs[pair]
                for i in range(4):
                    head = 4 * pair + i
                    part[b, :, head * 128:(head + 1) * 128] = out[i * 32:(i + 1) * 32, (i // 2) * 128:(i // 2 + 1) * 128]
            part[b, :, 1024:1152] = stat_tile(tops, 0) + stat_tile(sums, 8)
            core_copy(b).start()

            @pl.when(b >= 2)
            def _():
                x_copy(b - 2).start()

            if at_x[0] == j:
                @pl.when(n >= at_x[1])
                def _():
                    y_copy(n - at_x[1]).start()

            @pl.when(b >= LAG_Y)
            def _():
                send_mine(b - LAG_Y)
        return carry

    lax.fori_loop(0, N_BATCH, batch_step, 0)

    for b in range(N_SEQ, N_SEQ + LAG_F):
        if b - 2 < N_SEQ:
            core_copy(b - 2).wait_recv()
            merge_core(b - 2)
            x_copy(b - 2).start()
        if b - LAG_G < N_SEQ:
            forward(b - LAG_G, (b - LAG_G) % 2)
        if b - LAG_D < N_SEQ:
            forward_core(b - LAG_D, (b - LAG_D) % 2)
        if (b - LAG_X) % BATCH == 0 and (b - LAG_X) < N_SEQ:
            n = (b - LAG_X) // BATCH
            wait_x(n)
            project_out(n)
            y_copy(n).start()
        if (b - LAG_Y) % BATCH == 0 and (b - LAG_Y) < N_SEQ:
            n = (b - LAG_Y) // BATCH
            y_copy(n).wait_recv()
            add_peer(n)
        if b - LAG_Y < N_SEQ:
            send_mine(b - LAG_Y)
        c_copy(b - LAG_F).wait_recv()
        finish(b - LAG_F)

    def drain(b, carry):
        for copy in (core_copy(b), x_copy(b), gx_copy(b), gy_copy(b), diag_copy(b, 0), c_copy(b)):
            copy.wait_send()
        return carry

    def drain_y(n, carry):
        y_copy(n).wait_send()
        return carry

    lax.fori_loop(0, N_SEQ, drain, 0)
    lax.fori_loop(0, N_BATCH, drain_y, 0)


def block(q, k_rows, v_rows, hidden, w_o, k_cache, v_cache, prefix_len):
    rows = k_cache.shape[1] * 4
    vmem = pl.BlockSpec(memory_space=pltpu.VMEM)
    hbm = pl.BlockSpec(memory_space=pl.ANY)
    dma = pltpu.SemaphoreType.DMA
    return pl.pallas_call(
        block_kernel,
        out_shape=jax.ShapeDtypeStruct((N_SEQ, 32, 2048), jnp.bfloat16),
        in_specs=[pl.BlockSpec(memory_space=pltpu.SMEM), vmem, vmem, vmem, hbm, hbm, hbm, hbm],
        out_specs=vmem,
        scratch_shapes=[
            pltpu.VMEM((NBUF, rows, 128), jnp.bfloat16),
            pltpu.VMEM((NBUF, rows, 128), jnp.bfloat16),
            pltpu.VMEM((2, 2048, 128), jnp.float32),
            pltpu.VMEM((2, 32, 128), jnp.float32),
            pltpu.VMEM((2, 8, 128), jnp.float32),
            pltpu.VMEM((N_SEQ, 8, 1024), jnp.bfloat16),
            pltpu.VMEM((1024, 2048), jnp.bfloat16),
            pltpu.VMEM((N_SEQ, 32, 1152), jnp.float32),
            pltpu.VMEM((N_SEQ + 1, 16, 1152), jnp.float32),
            pltpu.VMEM((N_SEQ + BATCH, 16, 1152), jnp.float32),
            pltpu.VMEM((N_SEQ + BATCH, 8, 1152), jnp.float32),
            pltpu.VMEM((N_BATCH + 1, 2, BATCH * 8, 1024), jnp.float32),
            pltpu.VMEM((N_BATCH + 1, BATCH * 8, 1024), jnp.float32),
            pltpu.VMEM((N_SEQ + BATCH, 2, 4, 8, 1024), jnp.float32),
            dma((NBUF,)), dma((NBUF,)), dma, dma,
            dma((N_SEQ,)), dma((N_SEQ,)), dma((N_SEQ,)), dma((N_SEQ,)),
            dma((N_BATCH,)), dma((N_BATCH,)), *[dma((N_SEQ,))] * 8,
        ],
        compiler_params=pltpu.CompilerParams(vmem_limit_bytes=60 * 1024 * 1024, collective_id=0, has_side_effects=True),
        cost_estimate=pl.CostEstimate(flops=19_000_000_000, bytes_accessed=140_000_000, transcendentals=17_000_000),
    )(prefix_len, q, k_rows, v_rows, w_o, hidden, k_cache.reshape(N_SEQ, rows, 128), v_cache.reshape(N_SEQ, rows, 128))


def solution(mesh):
    def per_device(hidden, prefix_len, k_cache, v_cache, attn_norm, w_q, w_k, w_v, w_o, q_norm, k_norm):
        q, k_rows, v_rows = project(hidden, attn_norm, w_q, w_k, w_v, q_norm, k_norm, prefix_len)
        block_out = block(q.reshape(N_SEQ, 32, 1024), k_rows.reshape(N_SEQ, 128, 128), v_rows.reshape(N_SEQ, 128, 128), hidden, w_o, k_cache, v_cache, prefix_len)
        return block_out, k_rows.reshape(N_SEQ, 32, 4, 128), v_rows.reshape(N_SEQ, 32, 4, 128)

    cache_spec = P('dp', 'cp', 'tp', None)
    arg_specs = (P('dp', None, None), P('dp'), cache_spec, cache_spec, P(None), P(None, 'tp'), P(None, 'tp'), P(None, 'tp'), P('tp', None), P(None), P(None))
    out_specs = (P('dp', None, None), P('dp', None, 'tp', None), P('dp', None, 'tp', None))
    return jax.shard_map(per_device, mesh=mesh, in_specs=arg_specs, out_specs=out_specs, check_vma=False)
```

```python
import jax
import jax.numpy as jnp
import numpy as np
from jax import lax
from jax.experimental import pallas as pl
from jax.experimental.pallas import tpu as pltpu
from jax.sharding import PartitionSpec as P

HEAD_DIM = 128
NEG = -3e38
FLOOR = -1e38
LOG2E = 1.4426950408889634
NBUF = 4
CHUNK = 256
SCALE = HEAD_DIM ** -0.5 * LOG2E


def rope_tables(prefix_len):
    freq = (1.0 / 1e6 ** (np.arange(HEAD_DIM) % 64 / 64.0)).astype(np.float32)
    token_angles = np.arange(32, dtype=np.float32)[:, None] * freq
    wide = token_angles.astype(np.float64)
    off = np.concatenate([np.cos(wide), np.sin(wide)], axis=1).astype(np.float32)
    angles = prefix_len.astype(jnp.float32)[:, None] * freq
    return jnp.concatenate([jnp.cos(angles), jnp.sin(angles)], axis=1), jnp.asarray(off), jnp.asarray(freq[None])


def project_kernel(x_hbm, gain_ref, wq_ref, wk_ref, wv_ref, qn_ref, kn_ref, base_ref, off_ref, freq_ref, prefix_ref, q_out, k_out, v_out,
                   x_ref, normed, kf, vf, cos_t, sin_t, xsem):
    def load(m):
        return pltpu.make_async_copy(x_hbm.at[pl.ds(m * 256, 256)], x_ref.at[m], xsem.at[m])

    def prepare(m):
        load(m).wait()
        gain = gain_ref[...].astype(jnp.float32)
        for part in range(2):
            t = x_ref[m, part * 128:(part + 1) * 128, :].astype(jnp.float32)
            t = t * lax.rsqrt(jnp.mean(t * t, axis=1, keepdims=True) + 1e-6) * gain
            normed[m * 256 + part * 128:m * 256 + (part + 1) * 128, :] = t.astype(jnp.bfloat16)
        cb, sb = off_ref[:, :128], off_ref[:, 128:]
        freq = freq_ref[...]
        lane = lax.broadcasted_iota(jnp.int32, (32, 128), 1)
        token = lax.broadcasted_iota(jnp.int32, (32, 128), 0)
        token_angle = token.astype(jnp.float32) * freq
        for b in range(m * 8, m * 8 + 8):
            ca, sa = base_ref[b:b + 1, :128], base_ref[b:b + 1, 128:]
            prefix = prefix_ref[b]
            angle = (token + prefix).astype(jnp.float32) * freq
            base_angle = jnp.full((1, 128), prefix, jnp.int32).astype(jnp.float32) * freq
            eps = (angle - base_angle) - token_angle
            near = 1.0 - 0.5 * eps * eps
            ct, st = cb * near - sb * eps, sb * near + cb * eps
            sin = sa * ct + ca * st
            cos_t[b * 32:(b + 1) * 32, :] = ca * ct - sa * st
            sin_t[b * 32:(b + 1) * 32, :] = jnp.where(lane < 64, -sin, sin)

    def head(lin, gain, rows):
        t = lin.astype(jnp.bfloat16).astype(jnp.float32)
        t = t * lax.rsqrt(jnp.mean(t * t, axis=1, keepdims=True) + 1e-6) * gain
        return (t * cos_t[rows, :] + pltpu.roll(t, 64, 1) * sin_t[rows, :]).astype(jnp.bfloat16)

    def run(i, first, last):
        qg = qn_ref[...].astype(jnp.float32)
        kg = kn_ref[...].astype(jnp.float32)
        wkv = jnp.concatenate([wk_ref[...], wv_ref[...]], axis=1)
        if first:
            for m in range(4):
                load(m).start()

        def lines(m):
            if first:
                prepare(m)
            lhs = normed[m * 256:(m + 1) * 256, :]
            return jnp.dot(lhs, wq_ref[...], preferred_element_type=jnp.float32), jnp.dot(lhs, wkv, preferred_element_type=jnp.float32)

        ahead = lines(0)
        for m in range(4):
            (q, kv), ahead = ahead, lines(m + 1) if m < 3 else None
            rows = slice(m * 256, (m + 1) * 256)
            for g in range(2):
                q_out[rows, g * 128:(g + 1) * 128] = head(q[:, g * 128:(g + 1) * 128], qg, rows)
            spread = pl.ds(m * 1024 + i, 256, stride=4)
            kf[spread, :] = head(kv[:, :128], kg, rows).astype(jnp.float32)
            vf[spread, :] = kv[:, 128:]
            if last:
                done = slice(m * 1024, (m + 1) * 1024)
                k_out[done, :] = kf[done, :].astype(jnp.bfloat16)
                v_out[done, :] = vf[done, :].astype(jnp.bfloat16)

    i = pl.program_id(0)
    pl.when(i == 0)(lambda: run(0, True, False))
    pl.when((i > 0) & (i < 3))(lambda: run(i, False, False))
    pl.when(i == 3)(lambda: run(3, False, True))


def project(hidden, attn_norm, w_q, w_k, w_v, q_norm, k_norm, prefix_len):
    base, off, freq = rope_tables(prefix_len)
    whole = lambda shape: pl.BlockSpec(shape, lambda i: (0, 0))
    cols = lambda n, w: pl.BlockSpec((n, w), lambda i: (0, i))
    return pl.pallas_call(
        project_kernel,
        grid=(4,),
        out_shape=(jax.ShapeDtypeStruct((1024, 1024), jnp.bfloat16), jax.ShapeDtypeStruct((4096, 128), jnp.bfloat16), jax.ShapeDtypeStruct((4096, 128), jnp.bfloat16)),
        in_specs=[pl.BlockSpec(memory_space=pl.ANY), whole((1, 2048)), cols(2048, 256), cols(2048, 128), cols(2048, 128), whole((1, 128)), whole((1, 128)), whole((32, 256)), whole((32, 256)), whole((1, 128)), pl.BlockSpec(memory_space=pltpu.SMEM)],
        out_specs=(cols(1024, 256), whole((4096, 128)), whole((4096, 128))),
        scratch_shapes=[
            pltpu.VMEM((4, 256, 2048), jnp.bfloat16),
            pltpu.VMEM((1024, 2048), jnp.bfloat16),
            pltpu.VMEM((4096, 128), jnp.float32),
            pltpu.VMEM((4096, 128), jnp.float32),
            pltpu.VMEM((1024, 128), jnp.float32),
            pltpu.VMEM((1024, 128), jnp.float32),
            pltpu.SemaphoreType.DMA((4,)),
        ],
        compiler_params=pltpu.CompilerParams(vmem_limit_bytes=62 * 1024 * 1024),
        cost_estimate=pl.CostEstimate(flops=8_600_000_000, bytes_accessed=16_000_000, transcendentals=20_000),
    )(hidden.reshape(1024, 2048), attn_norm.reshape(1, 2048), w_q, w_k, w_v, q_norm.reshape(1, 128), k_norm.reshape(1, 128), base, off, freq, prefix_len)


def head_rows(ref, start, count, head):
    return ref[pl.ds(start * 4 + head, count, stride=4), :]


def pair_rows(ref, start, count, pair):
    return jnp.concatenate([head_rows(ref, start, count, 2 * pair), head_rows(ref, start, count, 2 * pair + 1)], axis=1)


def query_weights(q_ref, b, pair):
    def head(h):
        return jnp.concatenate([q_ref[b, :, (2 * h + g) * 128:(2 * h + g + 1) * 128] for g in range(2)], axis=0)
    zero = jnp.zeros((64, 128), jnp.bfloat16)
    top = jnp.concatenate([head(2 * pair), zero], axis=1)
    low = jnp.concatenate([zero, head(2 * pair + 1)], axis=1)
    return jnp.concatenate([top, low], axis=0).T


def masked_scores(keys, wq, mask):
    return jnp.where(mask, jnp.dot(keys, wq, preferred_element_type=jnp.float32), NEG)


def fold_rows(op, tensor):
    return op(tensor.reshape(tensor.shape[0] // 8, 8, 128), axis=0)


def attend_step(q_ref, kn_ref, vn_ref, kbuf, vbuf, scores, own_scores, tops, b, nxt, limit, own, between=()):
    row = lax.broadcasted_iota(jnp.int32, (CHUNK, 128), 0)
    wq = [query_weights(q_ref, nxt, pair) for pair in range(2)]
    new_top = [jnp.full((8, 128), FLOOR, jnp.float32) for _ in range(2)]
    total = [jnp.zeros((8, 128), jnp.float32) for _ in range(2)]
    out = [jnp.zeros((128, 256), jnp.float32) for _ in range(2)]

    def values(pair, s, vals):
        p = jnp.exp2((s - tops[pair]) * SCALE)
        total[pair] = total[pair] + fold_rows(jnp.sum, p)
        out[pair] = out[pair] + jnp.dot(p.astype(jnp.bfloat16).T, vals, preferred_element_type=jnp.float32)

    for c in range(2048 // CHUNK):
        rows = pl.ds(c * CHUNK, CHUNK)
        mask = row < limit - c * CHUNK
        for pair in range(2):
            if tops is not None:
                values(pair, scores[pair, rows, :], pair_rows(vbuf, c * CHUNK, CHUNK, pair))
            s = masked_scores(pair_rows(kbuf, c * CHUNK, CHUNK, pair), wq[pair], mask)
            scores[pair, rows, :] = s
            new_top[pair] = jnp.maximum(new_top[pair], fold_rows(jnp.max, s))
        for work in between[c::2048 // CHUNK]:
            work()
    token = lax.broadcasted_iota(jnp.int32, (32, 128), 1) % 32
    mask = lax.broadcasted_iota(jnp.int32, (32, 128), 0) <= token - own
    for pair in range(2):
        if tops is not None:
            values(pair, own_scores[pair], pair_rows(vn_ref.at[b], 0, 32, pair))
        s = masked_scores(pair_rows(kn_ref.at[nxt], 0, 32, pair), wq[pair], mask)
        own_scores[pair] = s
        new_top[pair] = jnp.maximum(new_top[pair], fold_rows(jnp.max, s))
    return out, [jnp.sum(t, axis=0, keepdims=True) for t in total], [jnp.max(t, axis=0, keepdims=True) for t in new_top]


def stat_tile(rows, lane0):
    lane = lax.broadcasted_iota(jnp.int32, (32, 128), 1)
    tile = jnp.zeros((32, 128), jnp.float32)
    for pair in range(2):
        col = jnp.broadcast_to(rows[pair], (128, 128)).T
        for i in range(4):
            tile = jnp.where(lane == lane0 + 4 * pair + i, col[i * 32:(i + 1) * 32], tile)
    return tile


N_SEQ = 32
BATCH = 2
N_BATCH = N_SEQ // BATCH
LAG_X, LAG_Y, LAG_G, LAG_D, LAG_F = 6, 9, 14, 18, 21
MESH = pl.DeviceIdType.MESH


def merge_parts(a, r):
    sa, sr = a[:, 1024:], r[:, 1024:]
    lane = lax.broadcasted_iota(jnp.int32, sa.shape, 1)
    top = jnp.maximum(sa, sr)
    fa = jnp.where(lane < 8, jnp.exp2((sa - top) * SCALE), 0.0)
    fr = jnp.where(lane < 8, jnp.exp2((sr - top) * SCALE), 0.0)
    total = sa * pltpu.roll(fa, 8, 1) + sr * pltpu.roll(fr, 8, 1)
    parts = []
    for h in range(8):
        cols = slice(h * 128, (h + 1) * 128)
        parts.append(a[:, cols] * fa[:, h:h + 1] + r[:, cols] * fr[:, h:h + 1])
    return parts, jnp.where(lane < 8, top, total)


def block_kernel(prefix_ref, q_ref, kn_ref, vn_ref, wo_hbm, x_hbm, k_hbm, v_hbm, out_ref,
                 kbuf, vbuf, scores, own_scores, tops_ref, x_ref, wo_ref, part, part_in, half, half_in, proj, proj_in, gath,
                 ksem, vsem, xsem, wsem, d_send, d_recv, x_send, x_recv, y_send, y_recv, gx_send, gx_recv, gy_send, gy_recv,
                 g_send, g_recv, c_send, c_recv):
    dp, tp, cp = lax.axis_index('dp'), lax.axis_index('tp'), lax.axis_index('cp')
    x, k = cp // 2, cp % 2
    core_peer = (dp, tp, cp + 1 - 2 * k)
    x_peer = (dp, tp, cp + 2 - 4 * x)
    y_peer = (dp, 1 - tp, cp)

    barrier = pltpu.get_barrier_semaphore()
    for peer in (core_peer, x_peer, y_peer):
        pl.semaphore_signal(barrier, inc=1, device_id=peer, device_id_type=MESH)

    def copies(b):
        slot = lax.rem(b, NBUF)
        return (pltpu.make_async_copy(k_hbm.at[b], kbuf.at[slot], ksem.at[slot]),
                pltpu.make_async_copy(v_hbm.at[b], vbuf.at[slot], vsem.at[slot]))

    def remote(src, dst, send, recv, peer):
        return pltpu.make_async_remote_copy(src_ref=src, dst_ref=dst, send_sem=send, recv_sem=recv, device_id=peer, device_id_type=MESH)

    def core_copy(b):
        return remote(part.at[b, pl.ds(pl.multiple_of((1 - k) * 16, 16), 16)], part_in.at[b], d_send.at[b], d_recv.at[b], core_peer)

    def x_copy(b):
        return remote(half.at[b, pl.ds(pl.multiple_of((1 - x) * 8, 8), 8)], half_in.at[b], x_send.at[b], x_recv.at[b], x_peer)

    def y_copy(n):
        return remote(proj.at[n, 1 - tp], proj_in.at[n], y_send.at[n], y_recv.at[n], y_peer)

    mine, from_x, from_y = x * 2 + tp, (1 - x) * 2 + tp, x * 2 + 1 - tp

    def gath_copy(s, slot, send, recv, peer):
        return remote(gath.at[s, k, slot], gath.at[s, k, slot], send.at[s], recv.at[s], peer)

    def gx_copy(s):
        return gath_copy(s, mine, gx_send, gx_recv, x_peer)

    def gy_copy(s):
        return gath_copy(s, mine, gy_send, gy_recv, y_peer)

    def diag_copy(s, odd):
        if odd:
            return gath_copy(s, from_x, g_send, g_recv, y_peer)
        return gath_copy(s, from_y, g_send, g_recv, x_peer)

    def c_copy(s):
        return remote(gath.at[s, k], gath.at[s, k], c_send.at[s], c_recv.at[s], core_peer)

    for b in range(NBUF - 1):
        for copy in copies(b):
            copy.start()
    own = jnp.where(cp == 3, 0, 64)

    first = k * 16 + x * 8
    x_load = pltpu.make_async_copy(x_hbm.at[:, pl.ds(pl.multiple_of(first, 8), 8), pl.ds(pl.multiple_of(tp * 1024, 1024), 1024)], x_ref, xsem)
    x_load.start()
    wo_load = pltpu.make_async_copy(wo_hbm, wo_ref, wsem)
    wo_load.start()

    def limit_of(b):
        return prefix_ref[b] - cp * 2048

    def keep_tops(tops):
        for pair in range(2):
            tops_ref[pair] = jnp.broadcast_to(tops[pair], (8, 128))

    copies(0)[0].wait()
    keep_tops(attend_step(q_ref, kn_ref, vn_ref, kbuf.at[0], None, scores, own_scores, None, 0, 0, limit_of(0), own)[2])
    pl.semaphore_wait(barrier, 3)
    x_load.wait()
    wo_load.wait()

    def merge_core(b):
        parts, stats = merge_parts(part[jnp.minimum(b, N_SEQ - 1), pl.ds(pl.multiple_of(k * 16, 16), 16), :], part_in[b])
        for h in range(8):
            half[b, :, h * 128:(h + 1) * 128] = parts[h]
        half[b, :, 1024:] = stats

    def wait_x(n):
        for i in range(BATCH):
            x_copy(n * BATCH + i).wait_recv()

    def normalized(n):
        seqs = pl.ds(n * BATCH, BATCH)
        a = half[seqs, pl.ds(pl.multiple_of(x * 8, 8), 8), :].reshape(BATCH * 8, 1152)
        r = half_in[seqs].reshape(BATCH * 8, 1152)
        parts, stats = merge_parts(a, r)
        inv = 1.0 / stats[:, 8:16]
        return jnp.concatenate([parts[h] * inv[:, h:h + 1] for h in range(8)], axis=1).astype(jnp.bfloat16)

    def project_part(n, o, y, q):
        lo = y * 1024 + q * 512
        proj[n, y, :, q * 512:(q + 1) * 512] = jnp.dot(o, wo_ref[:, lo:lo + 512], preferred_element_type=jnp.float32)

    def project_out(n):
        o = normalized(n)
        for y in range(2):
            for q in range(2):
                project_part(n, o, y, q)

    def add_peer(n):
        res = x_ref[pl.ds(jnp.minimum(n, N_BATCH - 1) * BATCH, BATCH)].reshape(BATCH * 8, 1024).astype(jnp.float32)
        gath[pl.ds(n * BATCH, BATCH), k, mine] = (proj[n, tp] + proj_in[n] + res).reshape(BATCH, 8, 1024)

    def send_mine(s):
        gy_copy(s).start()
        gx_copy(s).start()

    def forward(s, odd):
        gy_copy(s).wait_recv()
        gx_copy(s).wait_recv()
        diag_copy(s, odd).start()

    def forward_core(s, odd):
        diag_copy(s, odd).wait_recv()
        c_copy(s).start()

    def finish(s):
        at = jnp.minimum(s, N_SEQ - 1)
        for kk in range(2):
            for y in range(2):
                both = jnp.concatenate([gath[s, kk, y], gath[s, kk, 2 + y]], axis=0)
                out_ref[at, kk * 16:(kk + 1) * 16, y * 1024:(y + 1) * 1024] = both.astype(jnp.bfloat16)

    at_x, at_y = (divmod(lag, BATCH)[::-1] for lag in (LAG_X, LAG_Y))

    def batch_step(n, carry):
        def behind(at):
            return jnp.where(n >= at[1], n - at[1], N_BATCH)

        for j in range(BATCH):
            b = n * BATCH + j
            nxt = jnp.minimum(b + 1, N_SEQ - 1)

            def lagged(lag, b=b):
                return jnp.where(b >= lag, b - lag, N_SEQ)

            copies(b)[1].wait()

            @pl.when(b + 1 < N_SEQ)
            def _():
                copies(b + 1)[0].wait()

            @pl.when(b + NBUF - 1 < N_SEQ)
            def _():
                for copy in copies(b + NBUF - 1):
                    copy.start()

            @pl.when(b >= 2)
            def _():
                core_copy(b - 2).wait_recv()

            if at_x[0] == j:
                @pl.when(n >= at_x[1])
                def _():
                    wait_x(n - at_x[1])
            if at_y[0] == j:
                @pl.when(n >= at_y[1])
                def _():
                    y_copy(n - at_y[1]).wait_recv()

            @pl.when(b >= LAG_G)
            def _():
                forward(b - LAG_G, (j - LAG_G) % 2)

            @pl.when(b >= LAG_D)
            def _():
                forward_core(b - LAG_D, (j - LAG_D) % 2)

            @pl.when(b >= LAG_F)
            def _():
                c_copy(b - LAG_F).wait_recv()

            between = [lambda b=b: merge_core(lagged(2, b)), lambda b=b: finish(lagged(LAG_F, b))]
            if at_y[0] == j:
                between.append(lambda: add_peer(behind(at_y)))
            if at_x[0] == j:
                parts_of = normalized(behind(at_x))
                between += [lambda y=y, q=q: project_part(behind(at_x), parts_of, y, q) for y in range(2) for q in range(2)]
            tops = [tops_ref[pair, 0:1, :] for pair in range(2)]
            outs, sums, new_tops = attend_step(q_ref, kn_ref, vn_ref, kbuf.at[lax.rem(nxt, NBUF)], vbuf.at[lax.rem(b, NBUF)], scores, own_scores,
                                               tops, b, nxt, limit_of(nxt), own, between)
            keep_tops(new_tops)
            for pair in range(2):
                out = outs[pair]
                for i in range(4):
                    head = 4 * pair + i
                    part[b, :, head * 128:(head + 1) * 128] = out[i * 32:(i + 1) * 32, (i // 2) * 128:(i // 2 + 1) * 128]
            part[b, :, 1024:1152] = stat_tile(tops, 0) + stat_tile(sums, 8)
            core_copy(b).start()

            @pl.when(b >= 2)
            def _():
                x_copy(b - 2).start()

            if at_x[0] == j:
                @pl.when(n >= at_x[1])
                def _():
                    y_copy(n - at_x[1]).start()

            @pl.when(b >= LAG_Y)
            def _():
                send_mine(b - LAG_Y)
        return carry

    lax.fori_loop(0, N_BATCH, batch_step, 0)

    for b in range(N_SEQ, N_SEQ + LAG_F):
        if b - 2 < N_SEQ:
            core_copy(b - 2).wait_recv()
            merge_core(b - 2)
            x_copy(b - 2).start()
        if b - LAG_G < N_SEQ:
            forward(b - LAG_G, (b - LAG_G) % 2)
        if b - LAG_D < N_SEQ:
            forward_core(b - LAG_D, (b - LAG_D) % 2)
        if (b - LAG_X) % BATCH == 0 and (b - LAG_X) < N_SEQ:
            n = (b - LAG_X) // BATCH
            wait_x(n)
            project_out(n)
            y_copy(n).start()
        if (b - LAG_Y) % BATCH == 0 and (b - LAG_Y) < N_SEQ:
            n = (b - LAG_Y) // BATCH
            y_copy(n).wait_recv()
            add_peer(n)
        if b - LAG_Y < N_SEQ:
            send_mine(b - LAG_Y)
        c_copy(b - LAG_F).wait_recv()
        finish(b - LAG_F)

    def drain(b, carry):
        for copy in (core_copy(b), x_copy(b), gx_copy(b), gy_copy(b), diag_copy(b, 0), c_copy(b)):
            copy.wait_send()
        return carry

    def drain_y(n, carry):
        y_copy(n).wait_send()
        return carry

    lax.fori_loop(0, N_SEQ, drain, 0)
    lax.fori_loop(0, N_BATCH, drain_y, 0)


def block(q, k_rows, v_rows, hidden, w_o, k_cache, v_cache, prefix_len):
    rows = k_cache.shape[1] * 4
    vmem = pl.BlockSpec(memory_space=pltpu.VMEM)
    hbm = pl.BlockSpec(memory_space=pl.ANY)
    dma = pltpu.SemaphoreType.DMA
    return pl.pallas_call(
        block_kernel,
        out_shape=pltpu.VMEM((N_SEQ, 32, 2048), jnp.bfloat16),
        in_specs=[pl.BlockSpec(memory_space=pltpu.SMEM), vmem, vmem, vmem, hbm, hbm, hbm, hbm],
        out_specs=vmem,
        scratch_shapes=[
            pltpu.VMEM((NBUF, rows, 128), jnp.bfloat16),
            pltpu.VMEM((NBUF, rows, 128), jnp.bfloat16),
            pltpu.VMEM((2, 2048, 128), jnp.float32),
            pltpu.VMEM((2, 32, 128), jnp.float32),
            pltpu.VMEM((2, 8, 128), jnp.float32),
            pltpu.VMEM((N_SEQ, 8, 1024), jnp.bfloat16),
            pltpu.VMEM((1024, 2048), jnp.bfloat16),
            pltpu.VMEM((N_SEQ, 32, 1152), jnp.float32),
            pltpu.VMEM((N_SEQ + 1, 16, 1152), jnp.float32),
            pltpu.VMEM((N_SEQ + BATCH, 16, 1152), jnp.float32),
            pltpu.VMEM((N_SEQ + BATCH, 8, 1152), jnp.float32),
            pltpu.VMEM((N_BATCH + 1, 2, BATCH * 8, 1024), jnp.float32),
            pltpu.VMEM((N_BATCH + 1, BATCH * 8, 1024), jnp.float32),
            pltpu.VMEM((N_SEQ + BATCH, 2, 4, 8, 1024), jnp.float32),
            dma((NBUF,)), dma((NBUF,)), dma, dma,
            dma((N_SEQ,)), dma((N_SEQ,)), dma((N_SEQ,)), dma((N_SEQ,)),
            dma((N_BATCH,)), dma((N_BATCH,)), *[dma((N_SEQ,))] * 8,
        ],
        compiler_params=pltpu.CompilerParams(vmem_limit_bytes=56 * 1024 * 1024, collective_id=0, has_side_effects=True),
        cost_estimate=pl.CostEstimate(flops=19_000_000_000, bytes_accessed=140_000_000, transcendentals=17_000_000),
    )(prefix_len, q, k_rows, v_rows, w_o, hidden, k_cache.reshape(N_SEQ, rows, 128), v_cache.reshape(N_SEQ, rows, 128))


def solution(mesh):
    def per_device(hidden, prefix_len, k_cache, v_cache, attn_norm, w_q, w_k, w_v, w_o, q_norm, k_norm):
        q, k_rows, v_rows = project(hidden, attn_norm, w_q, w_k, w_v, q_norm, k_norm, prefix_len)
        block_out = block(q.reshape(N_SEQ, 32, 1024), k_rows.reshape(N_SEQ, 128, 128), v_rows.reshape(N_SEQ, 128, 128), hidden, w_o, k_cache, v_cache, prefix_len)
        return block_out, k_rows.reshape(N_SEQ, 32, 4, 128), v_rows.reshape(N_SEQ, 32, 4, 128)

    cache_spec = P('dp', 'cp', 'tp', None)
    arg_specs = (P('dp', None, None), P('dp'), cache_spec, cache_spec, P(None), P(None, 'tp'), P(None, 'tp'), P(None, 'tp'), P('tp', None), P(None), P(None))
    out_specs = (P('dp', None, None), P('dp', None, 'tp', None), P('dp', None, 'tp', None))
    return jax.shard_map(per_device, mesh=mesh, in_specs=arg_specs, out_specs=out_specs, check_vma=False)
```

```python
import jax
import jax.numpy as jnp
import numpy as np
from jax import lax
from jax.experimental import pallas as pl
from jax.experimental.pallas import tpu as pltpu
from jax.sharding import PartitionSpec as P

HEAD_DIM = 128
NEG = -3e38
FLOOR = -1e38
LOG2E = 1.4426950408889634
NBUF = 4
CHUNK = 256
SCALE = HEAD_DIM ** -0.5 * LOG2E


def rope_tables(prefix_len):
    freq = (1.0 / 1e6 ** (np.arange(HEAD_DIM) % 64 / 64.0)).astype(np.float32)
    token_angles = np.arange(32, dtype=np.float32)[:, None] * freq
    wide = token_angles.astype(np.float64)
    off = np.concatenate([np.cos(wide), np.sin(wide)], axis=1).astype(np.float32)
    angles = prefix_len.astype(jnp.float32)[:, None] * freq
    return jnp.concatenate([jnp.cos(angles), jnp.sin(angles)], axis=1), jnp.asarray(off), jnp.asarray(freq[None])


def project_kernel(x_hbm, gain_ref, wq_ref, wk_ref, wv_ref, qn_ref, kn_ref, base_ref, off_ref, freq_ref, prefix_ref, q_out, k_out, v_out,
                   x_ref, normed, kf, vf, cos_t, sin_t, xsem):
    def load(m):
        return pltpu.make_async_copy(x_hbm.at[pl.ds(m * 256, 256)], x_ref.at[m], xsem.at[m])

    def prepare(m):
        load(m).wait()
        gain = gain_ref[...].astype(jnp.float32).reshape(1, 2048)
        for part in range(2):
            t = x_ref[m, part * 128:(part + 1) * 128, :].astype(jnp.float32)
            t = t * lax.rsqrt(jnp.mean(t * t, axis=1, keepdims=True) + 1e-6) * gain
            normed[m * 256 + part * 128:m * 256 + (part + 1) * 128, :] = t.astype(jnp.bfloat16)
        cb, sb = off_ref[:, :128], off_ref[:, 128:]
        freq = freq_ref[...]
        lane = lax.broadcasted_iota(jnp.int32, (32, 128), 1)
        token = lax.broadcasted_iota(jnp.int32, (32, 128), 0)
        token_angle = token.astype(jnp.float32) * freq
        for b in range(m * 8, m * 8 + 8):
            ca, sa = base_ref[b:b + 1, :128], base_ref[b:b + 1, 128:]
            prefix = prefix_ref[b]
            angle = (token + prefix).astype(jnp.float32) * freq
            base_angle = jnp.full((1, 128), prefix, jnp.int32).astype(jnp.float32) * freq
            eps = (angle - base_angle) - token_angle
            near = 1.0 - 0.5 * eps * eps
            ct, st = cb * near - sb * eps, sb * near + cb * eps
            sin = sa * ct + ca * st
            cos_t[b * 32:(b + 1) * 32, :] = ca * ct - sa * st
            sin_t[b * 32:(b + 1) * 32, :] = jnp.where(lane < 64, -sin, sin)

    def head(lin, gain, rows):
        t = lin.astype(jnp.bfloat16).astype(jnp.float32)
        t = t * lax.rsqrt(jnp.mean(t * t, axis=1, keepdims=True) + 1e-6) * gain
        return (t * cos_t[rows, :] + pltpu.roll(t, 64, 1) * sin_t[rows, :]).astype(jnp.bfloat16)

    def run(i, first, last):
        qg = qn_ref[...].astype(jnp.float32)
        kg = kn_ref[...].astype(jnp.float32)
        wkv = jnp.concatenate([wk_ref[...], wv_ref[...]], axis=1)
        if first:
            for m in range(4):
                load(m).start()

        def lines(m):
            if first:
                prepare(m)
            lhs = normed[m * 256:(m + 1) * 256, :]
            return jnp.dot(lhs, wq_ref[...], preferred_element_type=jnp.float32), jnp.dot(lhs, wkv, preferred_element_type=jnp.float32)

        ahead = lines(0)
        for m in range(4):
            (q, kv), ahead = ahead, lines(m + 1) if m < 3 else None
            rows = slice(m * 256, (m + 1) * 256)
            for g in range(2):
                q_out[rows, g * 128:(g + 1) * 128] = head(q[:, g * 128:(g + 1) * 128], qg, rows)
            spread = pl.ds(m * 1024 + i, 256, stride=4)
            kf[spread, :] = head(kv[:, :128], kg, rows).astype(jnp.float32)
            vf[spread, :] = kv[:, 128:]
            if last:
                done = slice(m * 1024, (m + 1) * 1024)
                k_out[done, :] = kf[done, :].astype(jnp.bfloat16)
                v_out[done, :] = vf[done, :].astype(jnp.bfloat16)

    i = pl.program_id(0)
    pl.when(i == 0)(lambda: run(0, True, False))
    pl.when((i > 0) & (i < 3))(lambda: run(i, False, False))
    pl.when(i == 3)(lambda: run(3, False, True))


def project(hidden, attn_norm, w_q, w_k, w_v, q_norm, k_norm, prefix_len):
    base, off, freq = rope_tables(prefix_len)
    whole = lambda shape: pl.BlockSpec(shape, lambda i: (0, 0))
    cols = lambda n, w: pl.BlockSpec((n, w), lambda i: (0, i))
    return pl.pallas_call(
        project_kernel,
        grid=(4,),
        out_shape=(jax.ShapeDtypeStruct((1024, 1024), jnp.bfloat16), jax.ShapeDtypeStruct((4096, 128), jnp.bfloat16), jax.ShapeDtypeStruct((4096, 128), jnp.bfloat16)),
        in_specs=[pl.BlockSpec(memory_space=pl.ANY), pl.BlockSpec((2048,), lambda i: (0,)), cols(2048, 256), cols(2048, 128), cols(2048, 128), whole((1, 128)), whole((1, 128)), whole((32, 256)), whole((32, 256)), whole((1, 128)), pl.BlockSpec(memory_space=pltpu.SMEM)],
        out_specs=(cols(1024, 256), whole((4096, 128)), whole((4096, 128))),
        scratch_shapes=[
            pltpu.VMEM((4, 256, 2048), jnp.bfloat16),
            pltpu.VMEM((1024, 2048), jnp.bfloat16),
            pltpu.VMEM((4096, 128), jnp.float32),
            pltpu.VMEM((4096, 128), jnp.float32),
            pltpu.VMEM((1024, 128), jnp.float32),
            pltpu.VMEM((1024, 128), jnp.float32),
            pltpu.SemaphoreType.DMA((4,)),
        ],
        compiler_params=pltpu.CompilerParams(vmem_limit_bytes=62 * 1024 * 1024),
        cost_estimate=pl.CostEstimate(flops=8_600_000_000, bytes_accessed=16_000_000, transcendentals=20_000),
    )(hidden.reshape(1024, 2048), attn_norm, w_q, w_k, w_v, q_norm.reshape(1, 128), k_norm.reshape(1, 128), base, off, freq, prefix_len)


def head_rows(ref, start, count, head):
    return ref[pl.ds(start * 4 + head, count, stride=4), :]


def pair_rows(ref, start, count, pair):
    return jnp.concatenate([head_rows(ref, start, count, 2 * pair), head_rows(ref, start, count, 2 * pair + 1)], axis=1)


def query_weights(q_ref, b, pair):
    def head(h):
        return jnp.concatenate([q_ref[b, :, (2 * h + g) * 128:(2 * h + g + 1) * 128] for g in range(2)], axis=0)
    zero = jnp.zeros((64, 128), jnp.bfloat16)
    top = jnp.concatenate([head(2 * pair), zero], axis=1)
    low = jnp.concatenate([zero, head(2 * pair + 1)], axis=1)
    return jnp.concatenate([top, low], axis=0).T


def masked_scores(keys, wq, mask):
    return jnp.where(mask, jnp.dot(keys, wq, preferred_element_type=jnp.float32), NEG)


def fold_rows(op, tensor):
    return op(tensor.reshape(tensor.shape[0] // 8, 8, 128), axis=0)


def attend_step(q_ref, kn_ref, vn_ref, kbuf, vbuf, scores, own_scores, tops, b, nxt, limit, own, between=()):
    row = lax.broadcasted_iota(jnp.int32, (CHUNK, 128), 0)
    wq = [query_weights(q_ref, nxt, pair) for pair in range(2)]
    new_top = [jnp.full((8, 128), FLOOR, jnp.float32) for _ in range(2)]
    total = [jnp.zeros((8, 128), jnp.float32) for _ in range(2)]
    out = [jnp.zeros((128, 256), jnp.float32) for _ in range(2)]

    def values(pair, s, vals):
        p = jnp.exp2((s - tops[pair]) * SCALE)
        total[pair] = total[pair] + fold_rows(jnp.sum, p)
        out[pair] = out[pair] + jnp.dot(p.astype(jnp.bfloat16).T, vals, preferred_element_type=jnp.float32)

    for c in range(2048 // CHUNK):
        rows = pl.ds(c * CHUNK, CHUNK)
        mask = row < limit - c * CHUNK
        for pair in range(2):
            if tops is not None:
                values(pair, scores[pair, rows, :], pair_rows(vbuf, c * CHUNK, CHUNK, pair))
            s = masked_scores(pair_rows(kbuf, c * CHUNK, CHUNK, pair), wq[pair], mask)
            scores[pair, rows, :] = s
            new_top[pair] = jnp.maximum(new_top[pair], fold_rows(jnp.max, s))
        for work in between[c::2048 // CHUNK]:
            work()
    token = lax.broadcasted_iota(jnp.int32, (32, 128), 1) % 32
    mask = lax.broadcasted_iota(jnp.int32, (32, 128), 0) <= token - own
    for pair in range(2):
        if tops is not None:
            values(pair, own_scores[pair], pair_rows(vn_ref.at[b], 0, 32, pair))
        s = masked_scores(pair_rows(kn_ref.at[nxt], 0, 32, pair), wq[pair], mask)
        own_scores[pair] = s
        new_top[pair] = jnp.maximum(new_top[pair], fold_rows(jnp.max, s))
    return out, [jnp.sum(t, axis=0, keepdims=True) for t in total], [jnp.max(t, axis=0, keepdims=True) for t in new_top]


def stat_tile(rows, lane0):
    lane = lax.broadcasted_iota(jnp.int32, (32, 128), 1)
    tile = jnp.zeros((32, 128), jnp.float32)
    for pair in range(2):
        col = jnp.broadcast_to(rows[pair], (128, 128)).T
        for i in range(4):
            tile = jnp.where(lane == lane0 + 4 * pair + i, col[i * 32:(i + 1) * 32], tile)
    return tile


N_SEQ = 32
BATCH = 2
N_BATCH = N_SEQ // BATCH
LAG_X, LAG_Y, LAG_G, LAG_D, LAG_F = 6, 9, 14, 18, 21
MESH = pl.DeviceIdType.MESH


def merge_parts(a, r):
    sa, sr = a[:, 1024:], r[:, 1024:]
    lane = lax.broadcasted_iota(jnp.int32, sa.shape, 1)
    top = jnp.maximum(sa, sr)
    fa = jnp.where(lane < 8, jnp.exp2((sa - top) * SCALE), 0.0)
    fr = jnp.where(lane < 8, jnp.exp2((sr - top) * SCALE), 0.0)
    total = sa * pltpu.roll(fa, 8, 1) + sr * pltpu.roll(fr, 8, 1)
    parts = []
    for h in range(8):
        cols = slice(h * 128, (h + 1) * 128)
        parts.append(a[:, cols] * fa[:, h:h + 1] + r[:, cols] * fr[:, h:h + 1])
    return parts, jnp.where(lane < 8, top, total)


def block_kernel(prefix_ref, q_hbm, kn_hbm, vn_hbm, wo_hbm, x_hbm, k_hbm, v_hbm, out_ref,
                 kbuf, vbuf, scores, own_scores, tops_ref, x_ref, wo_ref, q_ref, kn_ref, vn_ref, part, part_in, half, half_in, proj, proj_in, gath,
                 ksem, vsem, xsem, wsem, nsem, d_send, d_recv, x_send, x_recv, y_send, y_recv, gx_send, gx_recv, gy_send, gy_recv,
                 g_send, g_recv, c_send, c_recv):
    dp, tp, cp = lax.axis_index('dp'), lax.axis_index('tp'), lax.axis_index('cp')
    x, k = cp // 2, cp % 2
    core_peer = (dp, tp, cp + 1 - 2 * k)
    x_peer = (dp, tp, cp + 2 - 4 * x)
    y_peer = (dp, 1 - tp, cp)

    barrier = pltpu.get_barrier_semaphore()
    for peer in (core_peer, x_peer, y_peer):
        pl.semaphore_signal(barrier, inc=1, device_id=peer, device_id_type=MESH)

    def copies(b):
        slot = lax.rem(b, NBUF)
        return (pltpu.make_async_copy(k_hbm.at[b], kbuf.at[slot], ksem.at[slot]),
                pltpu.make_async_copy(v_hbm.at[b], vbuf.at[slot], vsem.at[slot]))

    def remote(src, dst, send, recv, peer):
        return pltpu.make_async_remote_copy(src_ref=src, dst_ref=dst, send_sem=send, recv_sem=recv, device_id=peer, device_id_type=MESH)

    def core_copy(b):
        return remote(part.at[b, pl.ds(pl.multiple_of((1 - k) * 16, 16), 16)], part_in.at[b], d_send.at[b], d_recv.at[b], core_peer)

    def x_copy(b):
        return remote(half.at[b, pl.ds(pl.multiple_of((1 - x) * 8, 8), 8)], half_in.at[b], x_send.at[b], x_recv.at[b], x_peer)

    def y_copy(n):
        return remote(proj.at[n, 1 - tp], proj_in.at[n], y_send.at[n], y_recv.at[n], y_peer)

    mine, from_x, from_y = x * 2 + tp, (1 - x) * 2 + tp, x * 2 + 1 - tp

    def gath_copy(s, slot, send, recv, peer):
        return remote(gath.at[s, k, slot], gath.at[s, k, slot], send.at[s], recv.at[s], peer)

    def gx_copy(s):
        return gath_copy(s, mine, gx_send, gx_recv, x_peer)

    def gy_copy(s):
        return gath_copy(s, mine, gy_send, gy_recv, y_peer)

    def diag_copy(s, odd):
        if odd:
            return gath_copy(s, from_x, g_send, g_recv, y_peer)
        return gath_copy(s, from_y, g_send, g_recv, x_peer)

    def c_copy(s):
        return remote(gath.at[s, k], gath.at[s, k], c_send.at[s], c_recv.at[s], core_peer)

    new_loads = [pltpu.make_async_copy(src, dst, nsem.at[i]) for i, (src, dst) in enumerate(((q_hbm, q_ref), (kn_hbm, kn_ref), (vn_hbm, vn_ref)))]
    copies(0)[0].start()
    for load in new_loads:
        load.start()
    copies(0)[1].start()
    for b in range(1, NBUF - 1):
        for copy in copies(b):
            copy.start()
    own = jnp.where(cp == 3, 0, 64)

    first = k * 16 + x * 8
    x_load = pltpu.make_async_copy(x_hbm.at[:, pl.ds(pl.multiple_of(first, 8), 8), pl.ds(pl.multiple_of(tp * 1024, 1024), 1024)], x_ref, xsem)
    x_load.start()
    wo_load = pltpu.make_async_copy(wo_hbm, wo_ref, wsem)
    wo_load.start()

    def limit_of(b):
        return prefix_ref[b] - cp * 2048

    def keep_tops(tops):
        for pair in range(2):
            tops_ref[pair] = jnp.broadcast_to(tops[pair], (8, 128))

    copies(0)[0].wait()
    for load in new_loads:
        load.wait()
    keep_tops(attend_step(q_ref, kn_ref, vn_ref, kbuf.at[0], None, scores, own_scores, None, 0, 0, limit_of(0), own)[2])
    pl.semaphore_wait(barrier, 3)
    x_load.wait()
    wo_load.wait()

    def merge_core(b):
        parts, stats = merge_parts(part[jnp.minimum(b, N_SEQ - 1), pl.ds(pl.multiple_of(k * 16, 16), 16), :], part_in[b])
        for h in range(8):
            half[b, :, h * 128:(h + 1) * 128] = parts[h]
        half[b, :, 1024:] = stats

    def wait_x(n):
        for i in range(BATCH):
            x_copy(n * BATCH + i).wait_recv()

    def normalized(n):
        seqs = pl.ds(n * BATCH, BATCH)
        a = half[seqs, pl.ds(pl.multiple_of(x * 8, 8), 8), :].reshape(BATCH * 8, 1152)
        r = half_in[seqs].reshape(BATCH * 8, 1152)
        parts, stats = merge_parts(a, r)
        inv = 1.0 / stats[:, 8:16]
        return jnp.concatenate([parts[h] * inv[:, h:h + 1] for h in range(8)], axis=1).astype(jnp.bfloat16)

    def project_part(n, o, y, q):
        lo = y * 1024 + q * 512
        proj[n, y, :, q * 512:(q + 1) * 512] = jnp.dot(o, wo_ref[:, lo:lo + 512], preferred_element_type=jnp.float32)

    def project_out(n):
        o = normalized(n)
        for y in range(2):
            for q in range(2):
                project_part(n, o, y, q)

    def add_peer(n):
        res = x_ref[pl.ds(jnp.minimum(n, N_BATCH - 1) * BATCH, BATCH)].reshape(BATCH * 8, 1024).astype(jnp.float32)
        gath[pl.ds(n * BATCH, BATCH), k, mine] = (proj[n, tp] + proj_in[n] + res).reshape(BATCH, 8, 1024)

    def send_mine(s):
        gy_copy(s).start()
        gx_copy(s).start()

    def forward(s, odd):
        gy_copy(s).wait_recv()
        gx_copy(s).wait_recv()
        diag_copy(s, odd).start()

    def forward_core(s, odd):
        diag_copy(s, odd).wait_recv()
        c_copy(s).start()

    def finish(s):
        at = jnp.minimum(s, N_SEQ - 1)
        for kk in range(2):
            for y in range(2):
                both = jnp.concatenate([gath[s, kk, y], gath[s, kk, 2 + y]], axis=0)
                out_ref[at, kk * 16:(kk + 1) * 16, y * 1024:(y + 1) * 1024] = both.astype(jnp.bfloat16)

    at_x, at_y = (divmod(lag, BATCH)[::-1] for lag in (LAG_X, LAG_Y))

    def batch_step(n, carry):
        def behind(at):
            return jnp.where(n >= at[1], n - at[1], N_BATCH)

        for j in range(BATCH):
            b = n * BATCH + j
            nxt = jnp.minimum(b + 1, N_SEQ - 1)

            def lagged(lag, b=b):
                return jnp.where(b >= lag, b - lag, N_SEQ)

            copies(b)[1].wait()

            @pl.when(b + 1 < N_SEQ)
            def _():
                copies(b + 1)[0].wait()

            @pl.when(b + NBUF - 1 < N_SEQ)
            def _():
                for copy in copies(b + NBUF - 1):
                    copy.start()

            @pl.when(b >= 2)
            def _():
                core_copy(b - 2).wait_recv()

            if at_x[0] == j:
                @pl.when(n >= at_x[1])
                def _():
                    wait_x(n - at_x[1])
            if at_y[0] == j:
                @pl.when(n >= at_y[1])
                def _():
                    y_copy(n - at_y[1]).wait_recv()

            @pl.when(b >= LAG_G)
            def _():
                forward(b - LAG_G, (j - LAG_G) % 2)

            @pl.when(b >= LAG_D)
            def _():
                forward_core(b - LAG_D, (j - LAG_D) % 2)

            @pl.when(b >= LAG_F)
            def _():
                c_copy(b - LAG_F).wait_recv()

            between = [lambda b=b: merge_core(lagged(2, b)), lambda b=b: finish(lagged(LAG_F, b))]
            if at_y[0] == j:
                between.append(lambda: add_peer(behind(at_y)))
            if at_x[0] == j:
                parts_of = normalized(behind(at_x))
                between += [lambda y=y, q=q: project_part(behind(at_x), parts_of, y, q) for y in range(2) for q in range(2)]
            tops = [tops_ref[pair, 0:1, :] for pair in range(2)]
            outs, sums, new_tops = attend_step(q_ref, kn_ref, vn_ref, kbuf.at[lax.rem(nxt, NBUF)], vbuf.at[lax.rem(b, NBUF)], scores, own_scores,
                                               tops, b, nxt, limit_of(nxt), own, between)
            keep_tops(new_tops)
            for pair in range(2):
                out = outs[pair]
                for i in range(4):
                    head = 4 * pair + i
                    part[b, :, head * 128:(head + 1) * 128] = out[i * 32:(i + 1) * 32, (i // 2) * 128:(i // 2 + 1) * 128]
            part[b, :, 1024:1152] = stat_tile(tops, 0) + stat_tile(sums, 8)
            core_copy(b).start()

            @pl.when(b >= 2)
            def _():
                x_copy(b - 2).start()

            if at_x[0] == j:
                @pl.when(n >= at_x[1])
                def _():
                    y_copy(n - at_x[1]).start()

            @pl.when(b >= LAG_Y)
            def _():
                send_mine(b - LAG_Y)
        return carry

    lax.fori_loop(0, N_BATCH, batch_step, 0)

    for b in range(N_SEQ, N_SEQ + LAG_F):
        if b - 2 < N_SEQ:
            core_copy(b - 2).wait_recv()
            merge_core(b - 2)
            x_copy(b - 2).start()
        if b - LAG_G < N_SEQ:
            forward(b - LAG_G, (b - LAG_G) % 2)
        if b - LAG_D < N_SEQ:
            forward_core(b - LAG_D, (b - LAG_D) % 2)
        if (b - LAG_X) % BATCH == 0 and (b - LAG_X) < N_SEQ:
            n = (b - LAG_X) // BATCH
            wait_x(n)
            project_out(n)
            y_copy(n).start()
        if (b - LAG_Y) % BATCH == 0 and (b - LAG_Y) < N_SEQ:
            n = (b - LAG_Y) // BATCH
            y_copy(n).wait_recv()
            add_peer(n)
        if b - LAG_Y < N_SEQ:
            send_mine(b - LAG_Y)
        c_copy(b - LAG_F).wait_recv()
        finish(b - LAG_F)

    def drain(b, carry):
        for copy in (core_copy(b), x_copy(b), gx_copy(b), gy_copy(b), diag_copy(b, 0), c_copy(b)):
            copy.wait_send()
        return carry

    def drain_y(n, carry):
        y_copy(n).wait_send()
        return carry

    lax.fori_loop(0, N_SEQ, drain, 0)
    lax.fori_loop(0, N_BATCH, drain_y, 0)


def block(q, k_rows, v_rows, hidden, w_o, k_cache, v_cache, prefix_len):
    rows = k_cache.shape[1] * 4
    vmem = pl.BlockSpec(memory_space=pltpu.VMEM)
    hbm = pl.BlockSpec(memory_space=pl.ANY)
    dma = pltpu.SemaphoreType.DMA
    return pl.pallas_call(
        block_kernel,
        out_shape=pltpu.VMEM((N_SEQ, 32, 2048), jnp.bfloat16),
        in_specs=[pl.BlockSpec(memory_space=pltpu.SMEM), *[hbm] * 7],
        out_specs=vmem,
        scratch_shapes=[
            pltpu.VMEM((NBUF, rows, 128), jnp.bfloat16),
            pltpu.VMEM((NBUF, rows, 128), jnp.bfloat16),
            pltpu.VMEM((2, 2048, 128), jnp.float32),
            pltpu.VMEM((2, 32, 128), jnp.float32),
            pltpu.VMEM((2, 8, 128), jnp.float32),
            pltpu.VMEM((N_SEQ, 8, 1024), jnp.bfloat16),
            pltpu.VMEM((1024, 2048), jnp.bfloat16),
            pltpu.VMEM((N_SEQ, 32, 1024), jnp.bfloat16),
            pltpu.VMEM((N_SEQ, 128, 128), jnp.bfloat16),
            pltpu.VMEM((N_SEQ, 128, 128), jnp.bfloat16),
            pltpu.VMEM((N_SEQ, 32, 1152), jnp.float32),
            pltpu.VMEM((N_SEQ + 1, 16, 1152), jnp.float32),
            pltpu.VMEM((N_SEQ + BATCH, 16, 1152), jnp.float32),
            pltpu.VMEM((N_SEQ + BATCH, 8, 1152), jnp.float32),
            pltpu.VMEM((N_BATCH + 1, 2, BATCH * 8, 1024), jnp.float32),
            pltpu.VMEM((N_BATCH + 1, BATCH * 8, 1024), jnp.float32),
            pltpu.VMEM((N_SEQ + BATCH, 2, 4, 8, 1024), jnp.float32),
            dma((NBUF,)), dma((NBUF,)), dma, dma, dma((3,)),
            dma((N_SEQ,)), dma((N_SEQ,)), dma((N_SEQ,)), dma((N_SEQ,)),
            dma((N_BATCH,)), dma((N_BATCH,)), *[dma((N_SEQ,))] * 8,
        ],
        compiler_params=pltpu.CompilerParams(vmem_limit_bytes=56 * 1024 * 1024, collective_id=0, has_side_effects=True),
        cost_estimate=pl.CostEstimate(flops=19_000_000_000, bytes_accessed=140_000_000, transcendentals=17_000_000),
    )(prefix_len, q, k_rows, v_rows, w_o, hidden, k_cache.reshape(N_SEQ, rows, 128), v_cache.reshape(N_SEQ, rows, 128))


def solution(mesh):
    def per_device(hidden, prefix_len, k_cache, v_cache, attn_norm, w_q, w_k, w_v, w_o, q_norm, k_norm):
        q, k_rows, v_rows = project(hidden, attn_norm, w_q, w_k, w_v, q_norm, k_norm, prefix_len)
        block_out = block(q.reshape(N_SEQ, 32, 1024), k_rows.reshape(N_SEQ, 128, 128), v_rows.reshape(N_SEQ, 128, 128), hidden, w_o, k_cache, v_cache, prefix_len)
        return block_out, k_rows.reshape(N_SEQ, 32, 4, 128), v_rows.reshape(N_SEQ, 32, 4, 128)

    cache_spec = P('dp', 'cp', 'tp', None)
    arg_specs = (P('dp', None, None), P('dp'), cache_spec, cache_spec, P(None), P(None, 'tp'), P(None, 'tp'), P(None, 'tp'), P('tp', None), P(None), P(None))
    out_specs = (P('dp', None, None), P('dp', None, 'tp', None), P('dp', None, 'tp', None))
    return jax.shard_map(per_device, mesh=mesh, in_specs=arg_specs, out_specs=out_specs, check_vma=False)
```
